128 devices in a mesh: gx: 8 (over x, z_lo), gy: 16 (over z_hi, y, core).
Axes of the slice: x: 4, y: 4, z: 4 (z_hi: 2, z_lo: 2; z = z_hi * 2 + z_lo), core: 2. Of those that a mesh axis runs over, the one named last changes fastest.
Arguments:
- position: float32 [2, 48, 96, 128], P(None, 'gx', 'gy'), may hold values from 0 to 1
- velocity: float32 [2, 48, 96, 128], P(None, 'gx', 'gy'), may hold values from -3 to 3
- other_accel: float32 [2, 48, 96, 128], P(None, 'gx', 'gy'), may hold values from -5 to 5
- phase_ids: int32 [48, 96, 128], P('gx', 'gy'), may hold values from 0 to 1, as said below
- counts: int32 [48, 96], P('gx', 'gy'), may hold values from 48 to 128, as said below
Outputs:
- new_position: float32 [2, 48, 96, 128], P(None, 'gx', 'gy')
- new_velocity: float32 [2, 48, 96, 128], P(None, 'gx', 'gy')
- pressure: float32 [48, 96, 128], P('gx', 'gy')
- monitor: float32 [4, 4], replicated
The draws below stay inside these ranges and needn't reach their ends.
Inputs may be any that keep to these rules, and one draw needn't show every extreme that they name: `counts`: each entry is the number of live slots of its cell; the live slots are the first ones of the cell; some cell holds 128. `phase_ids`: both phases occur among the live slots.
All inputs are finite; a program needn't handle non-finite values.
Results may differ from the reference program's by a relative error of at most 0.0001.
Values sent between devices are 32-bit elements; how exact they have to be, the bound alone decides.
No kernel may reach another device: no remote copies, remote signals or barrier semaphores. Data moves between devices by JAX's collectives and lax.ppermute only.
A program may use at most 64 MiB of HBM per device.

```python
import jax
import jax.numpy as jnp
from jax import lax

SLOTS = 128
ITERS = 4
CELLS_X = 48
CELLS_Y = 96


def draw_counts(key, part):
    values = jax.random.randint(key, (CELLS_X, CELLS_Y), 48, SLOTS + 1, dtype=jnp.int32)
    return values.at[0, 0].set(SLOTS)


def draw_phase_ids(key, part):
    values = jax.random.randint(key, (CELLS_X, CELLS_Y, SLOTS), 0, 2, dtype=jnp.int32)
    return values.at[0, 0, 0].set(0).at[0, 0, 1].set(1)


def block_scale(own_key, dims, pieces, smallest, largest):
    factor_of = 1.0
    for axis_at, parts in pieces:
        draws = jax.random.uniform(jax.random.fold_in(jax.random.fold_in(own_key, 6), axis_at), (parts,), jnp.float32, smallest / len(pieces), largest / len(pieces))
        factor_of = factor_of * jnp.repeat(jnp.exp(draws), dims[axis_at] // parts).reshape((-1,) + (1,) * (len(dims) - 1 - axis_at))
    return factor_of


def gaussian(own_key, dims, deviation, reach, split=(), kind=jnp.bfloat16):
    drawn = jax.random.normal(own_key, dims, jnp.float32) * deviation
    if len(split) > 0:
        drawn = block_scale(own_key, dims, split, -0.22, 0.18) * drawn
    return jnp.clip(drawn, min=-reach, max=reach).astype(kind)


def setup_inputs(seed: int = 0) -> dict:
    seeds = jax.random.split(jax.random.key(seed), 6)
    position = jnp.clip(1.0 * jax.random.uniform(seeds[0], (2, CELLS_X, CELLS_Y, SLOTS), jnp.float32) ** block_scale(seeds[0], (2, CELLS_X, CELLS_Y, SLOTS), ((1, 8), (2, 16)), -0.2, 0.2), 0.0, 1.0)
    velocity = gaussian(seeds[1], (2, CELLS_X, CELLS_Y, SLOTS), 0.5, 3.0, ((1, 8), (2, 16)), jnp.float32)
    other_accel = gaussian(seeds[2], (2, CELLS_X, CELLS_Y, SLOTS), 1.0, 5.0, ((1, 8), (2, 16)), jnp.float32)
    phase_ids = draw_phase_ids(jax.random.fold_in(seeds[5], 71), 0)
    counts = draw_counts(jax.random.fold_in(seeds[5], 71), 0)
    return {"position": position, "velocity": velocity, "other_accel": other_accel, "phase_ids": phase_ids, "counts": counts}


TIME_STEP = 0.05
KERNEL_NORM = 4.0 / (3.141592653589793 * 64.0)
REST_LIGHT = 1.2
REST_HEAVY = 1.5
STIFF_LIGHT = 100.0
STIFF_HEAVY = 200.0
MASS_LIGHT = 1.0
MASS_HEAVY = 1.5
SENTINEL = 1.0e30


def window_of(source, off_x, off_y, row_count, col_count):
    return source[1 + off_x:1 + off_x + row_count, 1 + off_y:1 + off_y + col_count]


def pair_sums(centers, padded_list, with_force):
    center_x, center_y = centers[0], centers[1]
    near_x, near_y, near_live = padded_list[0], padded_list[1], padded_list[2]
    row_count, col_count = center_x.shape[0], center_x.shape[1]
    total_a = jnp.zeros_like(center_x)
    total_b = jnp.zeros_like(center_x)
    for off_x in (-1, 0, 1):
        for off_y in (-1, 0, 1):
            other_x = window_of(near_x, off_x, off_y, row_count, col_count)
            other_y = window_of(near_y, off_x, off_y, row_count, col_count)
            other_live = window_of(near_live, off_x, off_y, row_count, col_count)
            diff_x = center_x[..., :, None] - (other_x[..., None, :] + off_x)
            diff_y = center_y[..., :, None] - (other_y[..., None, :] + off_y)
            intersection = jnp.maximum(1.0 - diff_x * diff_x - diff_y * diff_y, 0.0) * other_live[..., None, :]
            if with_force:
                other_term = window_of(padded_list[3], off_x, off_y, row_count, col_count)
                pair_coef = intersection * intersection * (centers[2][..., :, None] + other_term[..., None, :])
                total_a = total_a + jnp.sum(pair_coef * diff_x, axis=-1)
                total_b = total_b + jnp.sum(pair_coef * diff_y, axis=-1)
            else:
                total_a = total_a + jnp.sum(intersection * intersection * intersection, axis=-1)
    if with_force:
        return (total_a, total_b)
    return (total_a,)


def blocked(with_force, centers, padded_list, row_count):
    block_count = row_count // 2

    def one_block(block_index):
        first_row = block_index * 2
        center_part = tuple(lax.dynamic_slice_in_dim(source, first_row, 2, 0) for source in centers)
        padded_part = tuple(lax.dynamic_slice_in_dim(source, first_row, 4, 0) for source in padded_list)
        return pair_sums(center_part, padded_part, with_force)

    results = lax.map(one_block, jnp.arange(block_count, dtype=jnp.int32))
    return tuple(source.reshape((row_count,) + source.shape[2:]) for source in results)


def local_bounds(density_ratio, live_bool, heavy_bool):
    light_sel = live_bool & jnp.logical_not(heavy_bool)
    heavy_sel = live_bool & heavy_bool
    top_ratio = jnp.stack([jnp.max(jnp.where(light_sel, density_ratio, -SENTINEL)),
                           jnp.max(jnp.where(heavy_sel, density_ratio, -SENTINEL))])
    low_ratio = jnp.stack([jnp.min(jnp.where(light_sel, density_ratio, SENTINEL)),
                           jnp.min(jnp.where(heavy_sel, density_ratio, SENTINEL))])
    return top_ratio, low_ratio


def wrapped(source):
    return jnp.pad(source, ((1, 1), (1, 1), (0, 0)), mode="wrap")


def reference(position, velocity, other_accel, phase_ids, counts):
    slot_index = jnp.arange(position.shape[-1], dtype=jnp.int32)
    live_bool = slot_index[None, None, :] < counts[:, :, None]
    heavy_bool = phase_ids == 1
    live_mask = live_bool.astype(jnp.float32)
    rest_density = jnp.where(heavy_bool, REST_HEAVY, REST_LIGHT).astype(jnp.float32)
    stiffness = jnp.where(heavy_bool, STIFF_HEAVY, STIFF_LIGHT).astype(jnp.float32)
    particle_mass = jnp.where(heavy_bool, MASS_HEAVY, MASS_LIGHT).astype(jnp.float32)
    pressure = jnp.zeros_like(live_mask)
    accel_x = jnp.zeros_like(live_mask)
    accel_y = jnp.zeros_like(live_mask)
    monitor_rows = []
    row_total = position.shape[1]
    for iteration in range(ITERS):
        vel_x = velocity[0] + TIME_STEP * (other_accel[0] + accel_x)
        vel_y = velocity[1] + TIME_STEP * (other_accel[1] + accel_y)
        pos_x = position[0] + TIME_STEP * vel_x
        pos_y = position[1] + TIME_STEP * vel_y
        (density_sum,) = blocked(False, (pos_x, pos_y), (wrapped(pos_x), wrapped(pos_y), wrapped(live_mask)), row_total)
        density = KERNEL_NORM * density_sum
        density_ratio = density / rest_density
        top_ratio, low_ratio = local_bounds(density_ratio, live_bool, heavy_bool)
        relaxation = 1.0 / (1.0 + top_ratio - low_ratio)
        particle_relax = jnp.where(heavy_bool, relaxation[1], relaxation[0])
        pressure = live_mask * (pressure + stiffness * particle_relax * (density_ratio - 1.0))
        safe_density = jnp.where(live_bool, density, 1.0)
        press_term = jnp.where(live_bool, pressure / (safe_density * safe_density), 0.0)
        force_x, force_y = blocked(True, (pos_x, pos_y, press_term),
                                   (wrapped(pos_x), wrapped(pos_y), wrapped(live_mask), wrapped(press_term)), row_total)
        accel_x = live_mask * (6.0 * KERNEL_NORM / particle_mass) * force_x
        accel_y = live_mask * (6.0 * KERNEL_NORM / particle_mass) * force_y
        monitor_rows.append(jnp.concatenate([top_ratio, low_ratio]))
    new_vel_x = live_mask * (velocity[0] + TIME_STEP * (other_accel[0] + accel_x))
    new_vel_y = live_mask * (velocity[1] + TIME_STEP * (other_accel[1] + accel_y))
    new_pos_x = live_mask * (position[0] + TIME_STEP * new_vel_x)
    new_pos_y = live_mask * (position[1] + TIME_STEP * new_vel_y)
    return (jnp.stack([new_pos_x, new_pos_y]), jnp.stack([new_vel_x, new_vel_y]), pressure, jnp.stack(monitor_rows))
```

```python
import jax
import jax.numpy as jnp
import numpy as np
from jax import lax
from jax.experimental import pallas as pl
from jax.experimental.pallas import tpu as pltpu
from jax.sharding import Mesh
from jax.sharding import PartitionSpec as P

ITERS = 4
GX = ("gx_0", "gx_1")
GY = ("gy_0", "gy_1", "gy_2")

F32, BF16 = jnp.float32, jnp.bfloat16
OFFS = tuple((ox, oy) for ox in (-1, 0, 1) for oy in (-1, 0, 1))


def offset_masks():
    out = np.ones((9, 32, 128), np.float32)
    for k, (ox, oy) in enumerate(OFFS):
        for row in (6, 7, 12, 13, 14, 15, 18, 19, 20, 21, 22, 23):
            out[k, row] = (ox, oy)[row % 2]
        out[k, 31] = ox * ox + oy * oy
    return out


def rnd(v):
    return v.astype(BF16).astype(F32)


def row_iota():
    return lax.broadcasted_iota(jnp.int32, (8, 128), 0)


def cell_slabs(pos_ref, r, c, want_l=True, want_r=True):
    row = row_iota()
    x = jnp.broadcast_to(pos_ref[r, c, 0:1, :], (8, 128))
    y = jnp.broadcast_to(pos_ref[r, c, 1:2, :], (8, 128))
    v = jnp.where((row & 1) == 1, y, x)
    v1 = rnd(v)
    rest = v - v1
    v2 = rnd(rest)
    v3 = rest - v2
    n = x * x + y * y
    n1 = rnd(n)
    nrest = n - n1
    n2 = rnd(nrest)
    n3 = nrest - n2
    left = right = None
    if want_l:
        la = v1
        lb = jnp.where((row == 4) | (row == 5), 1.0, v2)
        lc = jnp.where((row >= 2) & (row <= 5), 1.0, v3)
        ld = jnp.where(row == 0, n1, jnp.where(row == 1, n2, jnp.where(row == 2, n3, 1.0)))
        left = jnp.concatenate([la, lb, lc, ld], axis=0)
    if want_r:
        t1, t2, t3 = 2.0 * v1, 2.0 * v2, 2.0 * v3
        ra = jnp.where(row < 2, t1, jnp.where(row < 4, t2, jnp.where(row < 6, t3, -2.0)))
        rb = ra
        rc = jnp.where(row < 4, t1, jnp.where(row < 6, t2, -2.0))
        rd = jnp.where(row < 3, -1.0, jnp.where(row == 3, -n1, jnp.where(row == 4, -n2, jnp.where(row == 5, -n3, jnp.where(row == 6, 1.0, -1.0)))))
        right = jnp.concatenate([ra, rb, rc, rd], axis=0)
    return left, right


def pair_rhs(r1, r2, mask):
    zero = jnp.zeros((32, 128), BF16)
    return jnp.concatenate(
        [jnp.concatenate([r1 * mask, zero], axis=1), jnp.concatenate([zero, r2 * mask], axis=1)], axis=0)


def pair_s(left_t, rhs):
    return jnp.dot(left_t, rhs, preferred_element_type=F32)


def fill_slabs(pos_ref, ls, rs, lo, hi, rlo, rhi):
    def body(r, carry):
        for c in range(lo, hi):
            left, right = cell_slabs(pos_ref, r, c)
            ls[r, c] = left
            if rlo <= c < rhi:
                rs[r, c] = right.astype(BF16)
        return carry
    lax.fori_loop(lo, hi, body, 0)


def fill_pairs(ls, lt, start, rows, cols, dr, dc, rbase, cbase):
    def body(i, carry):
        for j in range(cols):
            both = jnp.concatenate([ls[rbase + i, cbase + j], ls[rbase + i + dr, cbase + j + dc]], axis=0)
            lt[start + i * cols + j] = both.T.astype(BF16)
        return carry
    lax.fori_loop(0, rows, body, 0)


def density_pair(rs, lt, masks_ref, i1, i2, first, stride):
    r1, r2 = rs[i1[0], i1[1]], rs[i2[0], i2[1]]
    acc = jnp.zeros((8, 256), F32)
    for k, (ox, oy) in enumerate(OFFS):
        s = pair_s(lt[first + ox * stride + oy], pair_rhs(r1, r2, masks_ref[k]))
        w = jnp.maximum(s, 0.0)
        w3 = w * w * w
        acc = acc + w3.reshape(16, 8, 256).sum(axis=0)
    return acc.sum(axis=0, keepdims=True)

TIME_STEP = 0.05
KERNEL_NORM = 4.0 / (3.141592653589793 * 64.0)
SENTINEL = 1.0e30


def density_own(pos_ref, masks_ref, ls, rs, lt, store):
    fill_slabs(pos_ref, ls, rs, 1, 9, 2, 8)
    fill_pairs(ls, lt, 0, 5, 8, 3, 0, 1, 1)
    def body(b, carry):
        for a in range(3):
            row = density_pair(rs, lt, masks_ref, (a + 2, b + 2), (a + 5, b + 2), (a + 1) * 8 + b + 1, 8)
            store(a, b, row[:, :128])
            store(a + 3, b, row[:, 128:])
        return carry
    lax.fori_loop(0, 6, body, 0)


def kd_kernel(pos_ref, code_ref, masks_ref, dens_ref, bnd_ref, ls, rs, lt):
    def store(a, b, row):
        dens_ref[a, pl.ds(b, 1), :] = row
    density_own(pos_ref, masks_ref, ls, rs, lt, store)
    code = code_ref[...]
    ratio = dens_ref[...] * jnp.where(code == 2.0, KERNEL_NORM / 1.5, KERNEL_NORM / 1.2)
    picks = []
    for phase in (1.0, 2.0):
        picks.append(jnp.where(code == phase, ratio, -SENTINEL))
    for phase in (1.0, 2.0):
        picks.append(jnp.where(code == phase, -ratio, -SENTINEL))
    lane = lax.broadcasted_iota(jnp.int32, (1, 128), 1)
    out = jnp.zeros((1, 128), F32)
    for k, pick in enumerate(picks):
        top = pick.max(axis=0).max(axis=0, keepdims=True).max(axis=1, keepdims=True)
        out = jnp.where(lane == k, top, out)
    bnd_ref[...] = jnp.broadcast_to(out, (128, 128))


def term_rows(t_ref, r, c):
    row = row_iota() & 3
    a, b0, b1 = (jnp.broadcast_to(t_ref[k, r, pl.ds(c, 1), :], (8, 128)) for k in range(3))
    return jnp.where(row == 0, 1.0, jnp.where(row == 1, a, jnp.where(row == 2, b0, b1)))


def hi_lo(v):
    hi = rnd(v)
    return jnp.where(row_iota() < 4, hi, v - hi)


def cell_moments(pos_ref, t_ref, r, c):
    t = term_rows(t_ref, r, c)
    x = jnp.broadcast_to(pos_ref[r + 1, c + 1, 0:1, :], (8, 128))
    y = jnp.broadcast_to(pos_ref[r + 1, c + 1, 1:2, :], (8, 128))
    groups = [hi_lo(t)]
    for q in (x, y):
        for o in (-1.0, 0.0, 1.0):
            groups.append(hi_lo(t * (q + o)))
    return groups


def kf_kernel(pos_ref, dens_ref, code_ref, p_ref, masks_ref, s_ref, q_ref, ls, rs, lt, dn, tt, gt):
    fill_slabs(pos_ref, ls, rs, 0, 10, 1, 9)
    fill_pairs(ls, lt, 0, 5, 8, 3, 0, 1, 1)
    fill_pairs(ls, lt, 40, 3, 10, 7, 0, 0, 0)
    fill_pairs(ls, lt, 70, 8, 3, 0, 7, 1, 0)
    def top_bottom(h, carry):
        for u in range(2):
            c = h * 2 + u
            row = density_pair(rs, lt, masks_ref, (1, c + 1), (8, c + 1), 50 + c + 1, 10)
            dn[0, pl.ds(c, 1), :] = row[:, :128]
            dn[7, pl.ds(c, 1), :] = row[:, 128:]
        return carry
    lax.fori_loop(0, 4, top_bottom, 0)
    def left_right(h, carry):
        for u in range(2):
            a = h * 2 + u + 1
            row = density_pair(rs, lt, masks_ref, (a + 1, 1), (a + 1, 8), 70 + a * 3 + 1, 3)
            dn[a, pl.ds(0, 1), :] = row[:, :128]
            dn[a, pl.ds(7, 1), :] = row[:, 128:]
        return carry
    lax.fori_loop(0, 3, left_right, 0)
    for a in range(6):
        dn[a + 1, pl.ds(1, 6), :] = dens_ref[a]
    code = code_ref[...]
    live = code > 0.0
    heavy = code == 2.0
    density = KERNEL_NORM * dn[...]
    ratio = density * jnp.where(heavy, 1.0 / 1.5, 1.0 / 1.2)
    q = jnp.where(live, jnp.where(heavy, 200.0, 100.0) * (ratio - 1.0), 0.0)
    q_ref[...] = q
    safe = jnp.where(live, density, 1.0)
    inv = jnp.where(live, 1.0 / (safe * safe), 0.0)
    b = q * inv
    tt[0] = p_ref[...] * inv
    tt[1] = jnp.where(heavy, 0.0, b)
    tt[2] = jnp.where(heavy, b, 0.0)
    def moments(i, carry):
        for j in range(8):
            one = cell_moments(pos_ref, tt, i, j)
            two = cell_moments(pos_ref, tt, i + 3, j)
            tiles = [jnp.concatenate([g, h], axis=0) for g, h in zip(one, two)]
            gt[i * 8 + j] = jnp.concatenate(tiles, axis=0).astype(BF16)
        return carry
    lax.fori_loop(0, 5, moments, 0)
    row = row_iota()
    def forces(bcol, carry):
        for a in range(3):
            r1, r2 = rs[a + 2, bcol + 2], rs[a + 5, bcol + 2]
            acc = jnp.zeros((48, 256), F32)
            for k, (ox, oy) in enumerate(OFFS):
                p = (a + 1 + ox) * 8 + bcol + 1 + oy
                s = pair_s(lt[p], pair_rhs(r1, r2, masks_ref[k]))
                w = jnp.maximum(s, 0.0)
                w2 = w * w
                hi = w2.astype(BF16)
                lo = (w2 - hi.astype(F32)).astype(BF16)
                g = jnp.concatenate([gt[p, 0:16], gt[p, 32 + 16 * ox:48 + 16 * ox], gt[p, 80 + 16 * oy:96 + 16 * oy]], axis=0)
                acc = acc + jnp.dot(jnp.concatenate([g, g], axis=1), jnp.concatenate([hi, lo], axis=0), preferred_element_type=F32)
            for h in range(2):
                aa = a + 3 * h
                lanes = slice(128 * h, 128 * h + 128)
                sums = []
                for t in range(3):
                    m = acc[16 * t + 8 * h:16 * t + 8 * h + 8, lanes]
                    sums.append(m + jnp.concatenate([m[4:8], m[0:4]], axis=0))
                x = jnp.broadcast_to(pos_ref[aa + 2, bcol + 2, 0:1, :], (8, 128))
                y = jnp.broadcast_to(pos_ref[aa + 2, bcol + 2, 1:2, :], (8, 128))
                ex = x * sums[0] - sums[1]
                ey = y * sums[0] - sums[2]
                e = jnp.where(row < 4, ex, ey)
                e0 = jnp.where(row < 4, jnp.broadcast_to(ex[0:1], (8, 128)), jnp.broadcast_to(ey[0:1], (8, 128)))
                code_row = jnp.broadcast_to(code_ref[aa + 1, pl.ds(bcol + 1, 1), :], (8, 128))
                scale = 6.0 * KERNEL_NORM * TIME_STEP * TIME_STEP
                coef = jnp.where(code_row == 2.0, scale / 1.5, jnp.where(code_row == 1.0, scale, 0.0))
                s_ref[aa, bcol] = coef * (term_rows(tt, aa + 1, bcol + 1) * e0 + e)
        return carry
    lax.fori_loop(0, 6, forces, 0)


VM = pl.BlockSpec(memory_space=pltpu.VMEM)
LIMIT = 40 * 1024 * 1024


def call_kd(pos, code, masks, **kw):
    return pl.pallas_call(
        kd_kernel,
        out_shape=(jax.ShapeDtypeStruct((6, 6, 128), F32), jax.ShapeDtypeStruct((128, 128), F32)),
        in_specs=[VM] * 3, out_specs=(VM, VM),
        scratch_shapes=[pltpu.VMEM((10, 10, 32, 128), F32), pltpu.VMEM((10, 10, 32, 128), BF16), pltpu.VMEM((40, 128, 64), BF16)],
        compiler_params=pltpu.CompilerParams(vmem_limit_bytes=LIMIT),
        cost_estimate=pl.CostEstimate(flops=4_000_000_0, bytes_accessed=200_000, transcendentals=0),
        name="density", **kw)(pos, code, masks)


def call_kf(pos, dens, code8, p8, masks, **kw):
    return pl.pallas_call(
        kf_kernel,
        out_shape=(jax.ShapeDtypeStruct((6, 6, 8, 128), F32), jax.ShapeDtypeStruct((8, 8, 128), F32)),
        in_specs=[VM] * 5, out_specs=(VM, VM),
        scratch_shapes=[pltpu.VMEM((10, 10, 32, 128), F32), pltpu.VMEM((10, 10, 32, 128), BF16), pltpu.VMEM((94, 128, 64), BF16),
                        pltpu.VMEM((8, 8, 128), F32), pltpu.VMEM((3, 8, 8, 128), F32), pltpu.VMEM((40, 112, 128), BF16)],
        compiler_params=pltpu.CompilerParams(vmem_limit_bytes=LIMIT),
        cost_estimate=pl.CostEstimate(flops=8_000_000_00, bytes_accessed=400_000, transcendentals=0),
        name="force", **kw)(pos, dens, code8, p8, masks)


FAR = 2.0 ** 20


def padded(block, sides, width):
    for axis, dim in sides:
        count = lax.axis_size(axis)
        forward = [(i, (i + 1) % count) for i in range(count)]
        backward = [(target, source) for source, target in forward]
        low = lax.ppermute(lax.slice_in_dim(block, block.shape[dim] - width, None, axis=dim), axis, forward)
        high = lax.ppermute(lax.slice_in_dim(block, 0, width, axis=dim), axis, backward)
        block = jnp.concatenate([low, block, high], axis=dim)
    return block


def local(position, velocity, other_accel, phase_ids, counts):
    slot_index = jnp.arange(128, dtype=jnp.int32)
    live = slot_index[None, None, :] < counts[:, :, None]
    code = jnp.where(live, phase_ids + 1, 0).astype(F32)
    masks = jnp.asarray(offset_masks(), BF16)
    rest = position - 0.5 + TIME_STEP * (velocity + TIME_STEP * other_accel)
    base = jnp.stack([jnp.where(live, rest[0], FAR), jnp.where(live, rest[1], 0.0)], axis=2)
    first = padded(jnp.concatenate([base, code[:, :, None, :]], axis=2), ((GX, 0), (GY, 1)), 2)
    near = first[:, :, :2]
    code8 = first[1:9, 1:9, 2]
    pressure = jnp.zeros((8, 8, 128), F32)
    rows = []
    for iteration in range(ITERS):
        dens, bounds = call_kd(near, code, masks)
        seen = lax.all_to_all(bounds, GX + GY, 0, 0, tiled=True)
        sums, gain = call_kf(near, dens, code8, pressure, masks)
        top = seen.max(axis=0)
        row = jnp.concatenate([top[:2], -top[2:4]])
        relax = 1.0 / (1.0 + row[:2] - row[2:])
        pressure = pressure + jnp.where(code8 == 2.0, relax[1], relax[0]) * gain
        parts = sums.reshape(6, 6, 2, 4, 128)
        delta = parts[:, :, :, 1] + relax[0] * parts[:, :, :, 2] + relax[1] * parts[:, :, :, 3]
        rows.append(row)
        if iteration < ITERS - 1:
            near = padded(base + delta, ((GX, 0), (GY, 1)), 2)
    change = jnp.stack([delta[:, :, 0], delta[:, :, 1]]) * (1.0 / TIME_STEP)
    new_velocity = jnp.where(live, velocity + TIME_STEP * other_accel + change, 0.0)
    new_position = jnp.where(live, position + TIME_STEP * new_velocity, 0.0)
    return new_position, new_velocity, pressure[1:7, 1:7], jnp.stack(rows)


def solution(mesh):
    torus = Mesh(mesh.devices.reshape(4, 2, 2, 4, 2), ("gx_0", "gx_1", "gy_0", "gy_1", "gy_2"))
    in_specs = (
        P(None, GX, GY, None),
        P(None, GX, GY, None),
        P(None, GX, GY, None),
        P(GX, GY, None),
        P(GX, GY),
    )
    out_specs = (P(None, GX, GY, None), P(None, GX, GY, None), P(GX, GY, None), P())
    return jax.shard_map(local, mesh=torus, in_specs=in_specs, out_specs=out_specs, check_vma=False)
```

```python
import jax
import jax.numpy as jnp
import numpy as np
from jax import lax
from jax.experimental import pallas as pl
from jax.experimental.pallas import tpu as pltpu
from jax.sharding import Mesh
from jax.sharding import PartitionSpec as P

ITERS = 4
GX = ("gx_0", "gx_1")
GY = ("gy_0", "gy_1", "gy_2")
ALL = GX + GY

F32, BF16 = jnp.float32, jnp.bfloat16
OFFS = tuple((ox, oy) for ox in (-1, 0, 1) for oy in (-1, 0, 1))


def offset_masks():
    out = np.ones((9, 32, 128), np.float32)
    for k, (ox, oy) in enumerate(OFFS):
        for row in (6, 7, 12, 13, 14, 15, 18, 19, 20, 21, 22, 23):
            out[k, row] = (ox, oy)[row % 2]
        out[k, 31] = ox * ox + oy * oy
    return out


def rnd(v):
    return v.astype(BF16).astype(F32)


def row_iota():
    return lax.broadcasted_iota(jnp.int32, (8, 128), 0)


def cell_slabs(pos_ref, r, c, want_l=True, want_r=True):
    row = row_iota()
    x = jnp.broadcast_to(pos_ref[r, c, 0:1, :], (8, 128))
    y = jnp.broadcast_to(pos_ref[r, c, 1:2, :], (8, 128))
    v = jnp.where((row & 1) == 1, y, x)
    v1 = rnd(v)
    rest = v - v1
    v2 = rnd(rest)
    v3 = rest - v2
    n = x * x + y * y
    n1 = rnd(n)
    nrest = n - n1
    n2 = rnd(nrest)
    n3 = nrest - n2
    left = right = None
    if want_l:
        la = v1
        lb = jnp.where((row == 4) | (row == 5), 1.0, v2)
        lc = jnp.where((row >= 2) & (row <= 5), 1.0, v3)
        ld = jnp.where(row == 0, n1, jnp.where(row == 1, n2, jnp.where(row == 2, n3, 1.0)))
        left = jnp.concatenate([la, lb, lc, ld], axis=0)
    if want_r:
        t1, t2, t3 = 2.0 * v1, 2.0 * v2, 2.0 * v3
        ra = jnp.where(row < 2, t1, jnp.where(row < 4, t2, jnp.where(row < 6, t3, -2.0)))
        rb = ra
        rc = jnp.where(row < 4, t1, jnp.where(row < 6, t2, -2.0))
        rd = jnp.where(row < 3, -1.0, jnp.where(row == 3, -n1, jnp.where(row == 4, -n2, jnp.where(row == 5, -n3, jnp.where(row == 6, 1.0, -1.0)))))
        right = jnp.concatenate([ra, rb, rc, rd], axis=0)
    return left, right


def pair_rhs(r1, r2, mask):
    zero = jnp.zeros((32, 128), BF16)
    return jnp.concatenate(
        [jnp.concatenate([r1 * mask, zero], axis=1), jnp.concatenate([zero, r2 * mask], axis=1)], axis=0)


def pair_s(left_t, rhs):
    return jnp.dot(left_t, rhs, preferred_element_type=F32)


def fill_slabs(pos_ref, ls, rs, lo, hi, rlo, rhi):
    def body(r, carry):
        for c in range(lo, hi):
            left, right = cell_slabs(pos_ref, r, c, True, rlo <= c < rhi)
            ls[r, c] = left
            if rlo <= c < rhi:
                rs[r, c] = right.astype(BF16)
        return carry
    lax.fori_loop(lo, hi, body, 0)


def fill_pairs(ls, lt, start, rows, cols, dr, dc, rbase, cbase):
    for i in range(rows):
        for j in range(cols):
            both = jnp.concatenate([ls[rbase + i, cbase + j], ls[rbase + i + dr, cbase + j + dc]], axis=0)
            lt[start + i * cols + j] = both.T.astype(BF16)


def density_pair(rs, lt, masks_ref, i1, i2, first, stride):
    r1, r2 = rs[i1[0], i1[1]], rs[i2[0], i2[1]]
    acc = jnp.zeros((8, 256), F32)
    for k, (ox, oy) in enumerate(OFFS):
        s = pair_s(lt[first + ox * stride + oy], pair_rhs(r1, r2, masks_ref[k]))
        w = jnp.maximum(s, 0.0)
        w3 = w * w * w
        acc = acc + w3.reshape(16, 8, 256).sum(axis=0)
    return acc.sum(axis=0, keepdims=True)

TIME_STEP = 0.05
KERNEL_NORM = 4.0 / (3.141592653589793 * 64.0)
SENTINEL = 1.0e30


def density_own(pos_ref, masks_ref, ls, rs, lt, store):
    fill_slabs(pos_ref, ls, rs, 1, 9, 1, 9)
    fill_pairs(ls, lt, 0, 5, 8, 3, 0, 1, 1)
    def body(b, carry):
        for a in range(3):
            row = density_pair(rs, lt, masks_ref, (a + 2, b + 2), (a + 5, b + 2), (a + 1) * 8 + b + 1, 8)
            store(a, b, row[:, :128])
            store(a + 3, b, row[:, 128:])
        return carry
    lax.fori_loop(0, 6, body, 0)


def kd_kernel(pos_ref, code_ref, masks_ref, dens_ref, bnd_ref, lt, rs, ls):
    def store(a, b, row):
        dens_ref[a, pl.ds(b, 1), :] = row
    density_own(pos_ref, masks_ref, ls, rs, lt, store)
    code = code_ref[...]
    ratio = dens_ref[...] * jnp.where(code == 2.0, KERNEL_NORM / 1.5, KERNEL_NORM / 1.2)
    picks = []
    for phase in (1.0, 2.0):
        picks.append(jnp.where(code == phase, ratio, -SENTINEL))
    for phase in (1.0, 2.0):
        picks.append(jnp.where(code == phase, -ratio, -SENTINEL))
    lane = lax.broadcasted_iota(jnp.int32, (1, 128), 1)
    out = jnp.zeros((1, 128), F32)
    for k, pick in enumerate(picks):
        top = pick.max(axis=0).max(axis=0, keepdims=True).max(axis=1, keepdims=True)
        out = jnp.where(lane == k, top, out)
    bnd_ref[...] = jnp.broadcast_to(out, (128, 128))


def term_rows(t_ref, r, c):
    row = row_iota() & 3
    a, b0, b1 = (jnp.broadcast_to(t_ref[k, r, pl.ds(c, 1), :], (8, 128)) for k in range(3))
    return jnp.where(row == 0, 1.0, jnp.where(row == 1, a, jnp.where(row == 2, b0, b1)))


def hi_lo(v):
    hi = rnd(v)
    return jnp.where(row_iota() < 4, hi, v - hi)


def cell_moments(pos_ref, t_ref, r, c):
    t = term_rows(t_ref, r, c)
    x = jnp.broadcast_to(pos_ref[r + 1, c + 1, 0:1, :], (8, 128))
    y = jnp.broadcast_to(pos_ref[r + 1, c + 1, 1:2, :], (8, 128))
    groups = [hi_lo(t)]
    for q in (x, y):
        for o in (-1.0, 0.0, 1.0):
            groups.append(hi_lo(t * (q + o)))
    return groups


def kf_kernel(pos_ref, dens_ref, code_ref, p_ref, masks_ref, lt0, rs, s_ref, q_ref, ls, lt, dn, tt, gt):
    fill_slabs(pos_ref, ls, None, 0, 10, 0, 0)
    fill_pairs(ls, lt, 0, 3, 10, 7, 0, 0, 0)
    fill_pairs(ls, lt, 30, 8, 3, 0, 7, 1, 0)
    def top_bottom(h, carry):
        for u in range(2):
            c = h * 2 + u
            row = density_pair(rs, lt, masks_ref, (1, c + 1), (8, c + 1), 10 + c + 1, 10)
            dn[0, pl.ds(c, 1), :] = row[:, :128]
            dn[7, pl.ds(c, 1), :] = row[:, 128:]
        return carry
    lax.fori_loop(0, 4, top_bottom, 0)
    def left_right(h, carry):
        for u in range(2):
            a = h * 2 + u + 1
            row = density_pair(rs, lt, masks_ref, (a + 1, 1), (a + 1, 8), 30 + a * 3 + 1, 3)
            dn[a, pl.ds(0, 1), :] = row[:, :128]
            dn[a, pl.ds(7, 1), :] = row[:, 128:]
        return carry
    lax.fori_loop(0, 3, left_right, 0)
    for a in range(6):
        dn[a + 1, pl.ds(1, 6), :] = dens_ref[a]
    code = code_ref[...]
    live = code > 0.0
    heavy = code == 2.0
    density = KERNEL_NORM * dn[...]
    ratio = density * jnp.where(heavy, 1.0 / 1.5, 1.0 / 1.2)
    q = jnp.where(live, jnp.where(heavy, 200.0, 100.0) * (ratio - 1.0), 0.0)
    q_ref[...] = q
    safe = jnp.where(live, density, 1.0)
    inv = jnp.where(live, 1.0 / (safe * safe), 0.0)
    b = q * inv
    tt[0] = p_ref[...] * inv
    tt[1] = jnp.where(heavy, 0.0, b)
    tt[2] = jnp.where(heavy, b, 0.0)
    def moments(i, carry):
        for j in range(8):
            one = cell_moments(pos_ref, tt, i, j)
            two = cell_moments(pos_ref, tt, i + 3, j)
            tiles = [jnp.concatenate([g, h], axis=0) for g, h in zip(one, two)]
            gt[i * 8 + j] = jnp.concatenate(tiles, axis=0).astype(BF16)
        return carry
    lax.fori_loop(0, 5, moments, 0)
    row = row_iota()
    def forces(bcol, carry):
        for a in range(3):
            r1, r2 = rs[a + 2, bcol + 2], rs[a + 5, bcol + 2]
            acc = jnp.zeros((48, 256), F32)
            for k, (ox, oy) in enumerate(OFFS):
                p = (a + 1 + ox) * 8 + bcol + 1 + oy
                s = pair_s(lt0[p], pair_rhs(r1, r2, masks_ref[k]))
                w = jnp.maximum(s, 0.0)
                w2 = w * w
                hi = w2.astype(BF16)
                lo = (w2 - hi.astype(F32)).astype(BF16)
                g = jnp.concatenate([gt[p, 0:16], gt[p, 32 + 16 * ox:48 + 16 * ox], gt[p, 80 + 16 * oy:96 + 16 * oy]], axis=0)
                acc = acc + jnp.dot(jnp.concatenate([g, g], axis=1), jnp.concatenate([hi, lo], axis=0), preferred_element_type=F32)
            for h in range(2):
                aa = a + 3 * h
                lanes = slice(128 * h, 128 * h + 128)
                sums = []
                for t in range(3):
                    m = acc[16 * t + 8 * h:16 * t + 8 * h + 8, lanes]
                    sums.append(m + jnp.concatenate([m[4:8], m[0:4]], axis=0))
                x = jnp.broadcast_to(pos_ref[aa + 2, bcol + 2, 0:1, :], (8, 128))
                y = jnp.broadcast_to(pos_ref[aa + 2, bcol + 2, 1:2, :], (8, 128))
                ex = x * sums[0] - sums[1]
                ey = y * sums[0] - sums[2]
                e = jnp.where(row < 4, ex, ey)
                e0 = jnp.where(row < 4, jnp.broadcast_to(ex[0:1], (8, 128)), jnp.broadcast_to(ey[0:1], (8, 128)))
                code_row = jnp.broadcast_to(code_ref[aa + 1, pl.ds(bcol + 1, 1), :], (8, 128))
                scale = 6.0 * KERNEL_NORM * TIME_STEP * TIME_STEP
                coef = jnp.where(code_row == 2.0, scale / 1.5, jnp.where(code_row == 1.0, scale, 0.0))
                out = coef * (term_rows(tt, aa + 1, bcol + 1) * e0 + e)
                for t in range(3):
                    s_ref[t, aa, bcol, 0:1, :] = out[t + 1:t + 2]
                    s_ref[t, aa, bcol, 1:2, :] = out[t + 5:t + 6]
        return carry
    lax.fori_loop(0, 6, forces, 0)


def kc_kernel(absolute, seen_ref, s_ref, base_ref, code_ref, p_ref, q_ref, pos_ref, pout_ref, row_ref):
    top = seen_ref[...].max(axis=0, keepdims=True)
    lane = lax.broadcasted_iota(jnp.int32, (1, 128), 1)
    top0, top1, neg0, neg1 = (jnp.sum(jnp.where(lane == k, top, 0.0), axis=1, keepdims=True) for k in range(4))
    row_ref[...] = jnp.where(lane < 2, top, -top)
    r0 = 1.0 / (1.0 + top0 + neg0)
    r1 = 1.0 / (1.0 + top1 + neg1)
    for a in range(8):
        pout_ref[a] = p_ref[a] + jnp.where(code_ref[a] == 2.0, r1, r0) * q_ref[a]
    for a in range(6):
        delta = s_ref[0, a] + r0[None] * s_ref[1, a] + r1[None] * s_ref[2, a]
        pos_ref[a] = base_ref[a] + delta if absolute else delta


VM = pl.BlockSpec(memory_space=pltpu.VMEM)
LIMIT = 20 * 1024 * 1024


def shaped(shape, dtype=F32):
    return jax.ShapeDtypeStruct(shape, dtype)


def call_kd(pos, code, masks):
    return pl.pallas_call(
        kd_kernel,
        out_shape=(shaped((6, 6, 128)), shaped((128, 128)), shaped((40, 128, 64), BF16), shaped((10, 10, 32, 128), BF16)),
        in_specs=[VM] * 3, out_specs=(VM,) * 4,
        scratch_shapes=[pltpu.VMEM((10, 10, 32, 128), F32)],
        compiler_params=pltpu.CompilerParams(vmem_limit_bytes=LIMIT),
        cost_estimate=pl.CostEstimate(flops=40_000_000, bytes_accessed=200_000, transcendentals=0),
        name="density")(pos, code, masks)


def call_kf(pos, dens, code8, p8, masks, pairs, rights):
    return pl.pallas_call(
        kf_kernel,
        out_shape=(shaped((3, 6, 6, 2, 128)), shaped((8, 8, 128))),
        in_specs=[VM] * 7, out_specs=(VM, VM),
        scratch_shapes=[pltpu.VMEM((10, 10, 32, 128), F32), pltpu.VMEM((54, 128, 64), BF16),
                        pltpu.VMEM((8, 8, 128), F32), pltpu.VMEM((3, 8, 8, 128), F32), pltpu.VMEM((40, 112, 128), BF16)],
        compiler_params=pltpu.CompilerParams(vmem_limit_bytes=LIMIT),
        cost_estimate=pl.CostEstimate(flops=800_000_000, bytes_accessed=400_000, transcendentals=0),
        name="force")(pos, dens, code8, p8, masks, pairs, rights)


def call_kc(seen, sums, base, code8, p8, gain, absolute):
    def kernel(*refs):
        kc_kernel(absolute, *refs)
    return pl.pallas_call(
        kernel,
        out_shape=(shaped((6, 6, 2, 128)), shaped((8, 8, 128)), shaped((1, 128))),
        in_specs=[VM] * 6, out_specs=(VM,) * 3,
        compiler_params=pltpu.CompilerParams(vmem_limit_bytes=LIMIT),
        cost_estimate=pl.CostEstimate(flops=1_000_000, bytes_accessed=400_000, transcendentals=0),
        name="combine")(seen.reshape(128, 128), sums, base, code8, p8, gain)


FAR = 2.0 ** 20
TILES = [(gx, gy) for gx in range(8) for gy in range(16)]


def home_of(gx, gy):
    return gx * 16 + gy


def work_of(gx, gy):
    x, flip = (gx, 0) if gx < 4 else (7 - gx, 1)
    chip = gy >> 1
    high = chip >> 2
    y = chip & 3 if high == 0 else 3 - (chip & 3)
    return ((x * 2 + (flip ^ high)) * 2 + high) * 8 + y * 2 + ((gx + gy) & 1)


def to_work(block):
    return lax.ppermute(block, ALL, [(home_of(gx, gy), work_of(gx, gy)) for gx, gy in TILES])


def to_home(block):
    return lax.ppermute(block, ALL, [(work_of(gx, gy), home_of(gx, gy)) for gx, gy in TILES])


def partners(dim, near):
    pairs = []
    for gx, gy in TILES:
        place, count = ((gx, 8), (gy, 16))[dim]
        other = (place + (1 if (place % 2 == 0) == near else -1)) % count
        pairs.append((work_of(gx, gy), work_of(*((other, gy) if dim == 0 else (gx, other)))))
    return pairs


def swapped(block, even, dim):
    first = lax.slice_in_dim(block, 0, 2, axis=dim)
    last = lax.slice_in_dim(block, 4, 6, axis=dim)
    far = lax.ppermute(jnp.where(even, first, last), ALL, partners(dim, False))
    near = lax.ppermute(jnp.where(even, last, first), ALL, partners(dim, True))
    low = jnp.where(even, far, near)
    high = jnp.where(even, near, far)
    return jnp.concatenate([low, block, high], axis=dim)


def padded(block):
    odd_x = lax.axis_index("gx_0") + lax.axis_index("gx_1") + lax.axis_index("gy_0")
    odd_y = odd_x + lax.axis_index("gy_2")
    return swapped(swapped(block, odd_x % 2 == 0, 0), odd_y % 2 == 0, 1)


def local(position, velocity, other_accel, phase_ids, counts):
    slot_index = jnp.arange(128, dtype=jnp.int32)
    live = slot_index[None, None, :] < counts[:, :, None]
    code = jnp.where(live, phase_ids + 1, 0).astype(F32)
    masks = jnp.asarray(offset_masks(), BF16)
    rest = position - 0.5 + TIME_STEP * (velocity + TIME_STEP * other_accel)
    base = jnp.stack([jnp.where(live, rest[0], FAR), jnp.where(live, rest[1], 0.0)], axis=2)
    packed = to_work(jnp.concatenate([base, code[:, :, None, :]], axis=2))
    base, code = packed[:, :, :2], packed[:, :, 2]
    first = padded(packed)
    near = first[:, :, :2]
    code8 = first[1:9, 1:9, 2]
    pressure = jnp.zeros((8, 8, 128), F32)
    rows = []
    for iteration in range(ITERS):
        dens, bounds, pairs, rights = call_kd(near, code, masks)
        seen = lax.all_to_all(bounds, ALL, 0, 0, tiled=True)
        sums, gain = call_kf(near, dens, code8, pressure, masks, pairs, rights)
        delta, pressure, row = call_kc(seen, sums, base, code8, pressure, gain, iteration < ITERS - 1)
        rows.append(row[0, :4])
        if iteration < ITERS - 1:
            near = padded(delta)
    result = to_home(jnp.concatenate([delta, pressure[1:7, 1:7, None]], axis=2))
    change = jnp.stack([result[:, :, 0], result[:, :, 1]]) * (1.0 / TIME_STEP)
    new_velocity = jnp.where(live, velocity + TIME_STEP * other_accel + change, 0.0)
    new_position = jnp.where(live, position + TIME_STEP * new_velocity, 0.0)
    return new_position, new_velocity, result[:, :, 2], jnp.stack(rows)


def solution(mesh):
    torus = Mesh(mesh.devices.reshape(4, 2, 2, 4, 2), ("gx_0", "gx_1", "gy_0", "gy_1", "gy_2"))
    in_specs = (
        P(None, GX, GY, None),
        P(None, GX, GY, None),
        P(None, GX, GY, None),
        P(GX, GY, None),
        P(GX, GY),
    )
    out_specs = (P(None, GX, GY, None), P(None, GX, GY, None), P(GX, GY, None), P())
    return jax.shard_map(local, mesh=torus, in_specs=in_specs, out_specs=out_specs, check_vma=False)
```

```python
import jax
import jax.numpy as jnp
import numpy as np
from jax import lax
from jax.experimental import pallas as pl
from jax.experimental.pallas import tpu as pltpu
from jax.sharding import Mesh
from jax.sharding import PartitionSpec as P

ITERS = 4
GX = ("gx_0", "gx_1")
GY = ("gy_0", "gy_1", "gy_2")
ALL = GX + GY

F32, BF16 = jnp.float32, jnp.bfloat16
OFFS = tuple((ox, oy) for ox in (-1, 0, 1) for oy in (-1, 0, 1))


def offset_masks():
    out = np.ones((9, 32, 128), np.float32)
    for k, (ox, oy) in enumerate(OFFS):
        for row in (6, 7, 12, 13, 14, 15, 18, 19, 20, 21, 22, 23):
            out[k, row] = (ox, oy)[row % 2]
        out[k, 31] = ox * ox + oy * oy
    return out


def rnd(v):
    return v.astype(BF16).astype(F32)


def row_iota():
    return lax.broadcasted_iota(jnp.int32, (8, 128), 0)


def cell_slabs(pos_ref, r, c, want_l=True, want_r=True):
    row = row_iota()
    x = jnp.broadcast_to(pos_ref[r, c, 0:1, :], (8, 128))
    y = jnp.broadcast_to(pos_ref[r, c, 1:2, :], (8, 128))
    v = jnp.where((row & 1) == 1, y, x)
    v1 = rnd(v)
    rest = v - v1
    v2 = rnd(rest)
    v3 = rest - v2
    n = x * x + y * y
    n1 = rnd(n)
    nrest = n - n1
    n2 = rnd(nrest)
    n3 = nrest - n2
    left = right = None
    if want_l:
        la = v1
        lb = jnp.where((row == 4) | (row == 5), 1.0, v2)
        lc = jnp.where((row >= 2) & (row <= 5), 1.0, v3)
        ld = jnp.where(row == 0, n1, jnp.where(row == 1, n2, jnp.where(row == 2, n3, 1.0)))
        left = jnp.concatenate([la, lb, lc, ld], axis=0)
    if want_r:
        t1, t2, t3 = 2.0 * v1, 2.0 * v2, 2.0 * v3
        ra = jnp.where(row < 2, t1, jnp.where(row < 4, t2, jnp.where(row < 6, t3, -2.0)))
        rb = ra
        rc = jnp.where(row < 4, t1, jnp.where(row < 6, t2, -2.0))
        rd = jnp.where(row < 3, -1.0, jnp.where(row == 3, -n1, jnp.where(row == 4, -n2, jnp.where(row == 5, -n3, jnp.where(row == 6, 1.0, -1.0)))))
        right = jnp.concatenate([ra, rb, rc, rd], axis=0)
    return left, right


def pair_rhs(r1, r2, mask):
    zero = jnp.zeros((32, 128), BF16)
    return jnp.concatenate(
        [jnp.concatenate([r1 * mask, zero], axis=1), jnp.concatenate([zero, r2 * mask], axis=1)], axis=0)


def pair_s(left_t, rhs):
    return jnp.dot(left_t, rhs, preferred_element_type=F32)


def fill_slabs(pos_ref, ls, rs, lo, hi, rlo, rhi):
    def body(r, carry):
        for c in range(lo, hi):
            left, right = cell_slabs(pos_ref, r, c, True, rlo <= c < rhi)
            ls[r, c] = left
            if rlo <= c < rhi:
                rs[r, c] = right.astype(BF16)
        return carry
    lax.fori_loop(lo, hi, body, 0)


def fill_pairs(ls, lt, start, rows, cols, dr, dc, rbase, cbase):
    for i in range(rows):
        for j in range(cols):
            both = jnp.concatenate([ls[rbase + i, cbase + j], ls[rbase + i + dr, cbase + j + dc]], axis=0)
            lt[start + i * cols + j] = both.T.astype(BF16)


def density_pair(rs, lt, masks_ref, i1, i2, first, stride, squares=None, at=0):
    r1, r2 = rs[i1[0], i1[1]], rs[i2[0], i2[1]]
    acc = jnp.zeros((8, 256), F32)
    for k, (ox, oy) in enumerate(OFFS):
        s = pair_s(lt[first + ox * stride + oy], pair_rhs(r1, r2, masks_ref[k]))
        w = jnp.maximum(s, 0.0)
        w2 = w * w
        if squares is not None:
            squares[at * 9 + k] = w2
        w3 = w2 * w
        acc = acc + w3.reshape(16, 8, 256).sum(axis=0)
    return acc.sum(axis=0, keepdims=True)


TIME_STEP = 0.05
KERNEL_NORM = 4.0 / (3.141592653589793 * 64.0)
SENTINEL = 1.0e30


def bounds_of(dens, code, bnd_ref):
    ratio = dens * jnp.where(code == 2.0, KERNEL_NORM / 1.5, KERNEL_NORM / 1.2)
    picks = []
    for phase in (1.0, 2.0):
        picks.append(jnp.where(code == phase, ratio, -SENTINEL))
    for phase in (1.0, 2.0):
        picks.append(jnp.where(code == phase, -ratio, -SENTINEL))
    lane = lax.broadcasted_iota(jnp.int32, (1, 128), 1)
    out = jnp.zeros((1, 128), F32)
    for k, pick in enumerate(picks):
        top = pick.max(axis=0).max(axis=0, keepdims=True).max(axis=1, keepdims=True)
        out = jnp.where(lane == k, top, out)
    bnd_ref[...] = jnp.broadcast_to(out, (128, 128))


def term_rows(t_ref, r, c):
    row = row_iota() & 3
    a, b0, b1 = (jnp.broadcast_to(t_ref[k, r, pl.ds(c, 1), :], (8, 128)) for k in range(3))
    return jnp.where(row == 0, 1.0, jnp.where(row == 1, a, jnp.where(row == 2, b0, b1)))


def hi_lo(v):
    hi = rnd(v)
    return jnp.where(row_iota() < 4, hi, v - hi)


def cell_moments(pos_ref, t_ref, r, c):
    t = term_rows(t_ref, r, c)
    x = jnp.broadcast_to(pos_ref[r + 1, c + 1, 0:1, :], (8, 128))
    y = jnp.broadcast_to(pos_ref[r + 1, c + 1, 1:2, :], (8, 128))
    groups = [hi_lo(t)]
    for q in (x, y):
        for o in (-1.0, 0.0, 1.0):
            groups.append(hi_lo(t * (q + o)))
    return groups


def kdf_kernel(pos_ref, base_ref, code_ref, own_ref, p_ref, masks_ref, bnd_ref, s_ref, q_ref, ls, rs, lt, dn, tt, gt, squares):
    fill_slabs(pos_ref, ls, rs, 0, 10, 1, 9)
    fill_pairs(ls, lt, 0, 5, 8, 3, 0, 1, 1)
    fill_pairs(ls, lt, 40, 3, 10, 7, 0, 0, 0)
    fill_pairs(ls, lt, 70, 8, 3, 0, 7, 1, 0)
    def own(b, carry):
        for a in range(3):
            row = density_pair(rs, lt, masks_ref, (a + 2, b + 2), (a + 5, b + 2), (a + 1) * 8 + b + 1, 8, squares, b * 3 + a)
            dn[a + 1, pl.ds(b + 1, 1), :] = row[:, :128]
            dn[a + 4, pl.ds(b + 1, 1), :] = row[:, 128:]
        return carry
    lax.fori_loop(0, 6, own, 0)
    def top_bottom(h, carry):
        for u in range(2):
            c = h * 2 + u
            row = density_pair(rs, lt, masks_ref, (1, c + 1), (8, c + 1), 50 + c + 1, 10)
            dn[0, pl.ds(c, 1), :] = row[:, :128]
            dn[7, pl.ds(c, 1), :] = row[:, 128:]
        return carry
    lax.fori_loop(0, 4, top_bottom, 0)
    def left_right(h, carry):
        for u in range(2):
            a = h * 2 + u + 1
            row = density_pair(rs, lt, masks_ref, (a + 1, 1), (a + 1, 8), 70 + a * 3 + 1, 3)
            dn[a, pl.ds(0, 1), :] = row[:, :128]
            dn[a, pl.ds(7, 1), :] = row[:, 128:]
        return carry
    lax.fori_loop(0, 3, left_right, 0)
    bounds_of(dn[...], own_ref[...], bnd_ref)
    code = code_ref[...]
    live = code > 0.0
    heavy = code == 2.0
    density = KERNEL_NORM * dn[...]
    ratio = density * jnp.where(heavy, 1.0 / 1.5, 1.0 / 1.2)
    q = jnp.where(live, jnp.where(heavy, 200.0, 100.0) * (ratio - 1.0), 0.0)
    q_ref[...] = q
    safe = jnp.where(live, density, 1.0)
    inv = jnp.where(live, 1.0 / (safe * safe), 0.0)
    b = q * inv
    tt[0] = p_ref[...] * inv
    tt[1] = jnp.where(heavy, 0.0, b)
    tt[2] = jnp.where(heavy, b, 0.0)
    def moments(i, carry):
        for j in range(8):
            one = cell_moments(pos_ref, tt, i, j)
            two = cell_moments(pos_ref, tt, i + 3, j)
            tiles = [jnp.concatenate([g, h], axis=0) for g, h in zip(one, two)]
            gt[i * 8 + j] = jnp.concatenate(tiles, axis=0).astype(BF16)
        return carry
    lax.fori_loop(0, 5, moments, 0)
    row = row_iota()
    def forces(step, carry):
        accs = [jnp.zeros((48, 256), F32) for _ in range(2)]
        work = [((2 * step + m) % 3, (2 * step + m) // 3) for m in range(2)]
        for k, (ox, oy) in enumerate(OFFS):
            for m in range(2):
                a, bcol = work[m]
                p = (a + 1 + ox) * 8 + bcol + 1 + oy
                w2 = squares[(2 * step + m) * 9 + k]
                hi = w2.astype(BF16)
                lo = (w2 - hi.astype(F32)).astype(BF16)
                g = jnp.concatenate([gt[p, 0:16], gt[p, 32 + 16 * ox:48 + 16 * ox], gt[p, 80 + 16 * oy:96 + 16 * oy]], axis=0)
                accs[m] = accs[m] + jnp.dot(jnp.concatenate([g, g], axis=1), jnp.concatenate([hi, lo], axis=0), preferred_element_type=F32)
        for m in range(2):
            a, bcol = work[m]
            acc = accs[m]
            for h in range(2):
                aa = a + 3 * h
                lanes = slice(128 * h, 128 * h + 128)
                sums = []
                for t in range(3):
                    m = acc[16 * t + 8 * h:16 * t + 8 * h + 8, lanes]
                    sums.append(m + jnp.concatenate([m[4:8], m[0:4]], axis=0))
                x = jnp.broadcast_to(pos_ref[aa + 2, bcol + 2, 0:1, :], (8, 128))
                y = jnp.broadcast_to(pos_ref[aa + 2, bcol + 2, 1:2, :], (8, 128))
                ex = x * sums[0] - sums[1]
                ey = y * sums[0] - sums[2]
                e = jnp.where(row < 4, ex, ey)
                e0 = jnp.where(row < 4, jnp.broadcast_to(ex[0:1], (8, 128)), jnp.broadcast_to(ey[0:1], (8, 128)))
                code_row = jnp.broadcast_to(code_ref[aa + 1, pl.ds(bcol + 1, 1), :], (8, 128))
                scale = 6.0 * KERNEL_NORM * TIME_STEP * TIME_STEP
                coef = jnp.where(code_row == 2.0, scale / 1.5, jnp.where(code_row == 1.0, scale, 0.0))
                out = coef * (term_rows(tt, aa + 1, bcol + 1) * e0 + e)
                s_ref[0, aa, bcol, 0:1, :] = base_ref[aa, bcol, 0:1, :] + out[1:2]
                s_ref[0, aa, bcol, 1:2, :] = base_ref[aa, bcol, 1:2, :] + out[5:6]
                for t in (1, 2):
                    s_ref[t, aa, bcol, 0:1, :] = out[t + 1:t + 2]
                    s_ref[t, aa, bcol, 1:2, :] = out[t + 5:t + 6]
        return carry
    lax.fori_loop(0, 9, forces, 0)


def kc_kernel(seen_ref, s_ref, code_ref, p_ref, q_ref, pos_ref, pout_ref, row_ref):
    top = seen_ref[...].max(axis=0, keepdims=True)
    lane = lax.broadcasted_iota(jnp.int32, (1, 128), 1)
    top0, top1, neg0, neg1 = (jnp.sum(jnp.where(lane == k, top, 0.0), axis=1, keepdims=True) for k in range(4))
    r0 = 1.0 / (1.0 + top0 + neg0)
    r1 = 1.0 / (1.0 + top1 + neg1)
    row_ref[...] = jnp.where(lane < 2, top, jnp.where(lane < 4, -top, jnp.where(lane == 4, r0, r1)))
    for a in range(8):
        pout_ref[a] = p_ref[a] + jnp.where(code_ref[a] == 2.0, r1, r0) * q_ref[a]
    for a in range(10):
        pos_ref[a] = s_ref[0, a] + r0[None] * s_ref[1, a] + r1[None] * s_ref[2, a]


VM = pl.BlockSpec(memory_space=pltpu.VMEM)


def shaped(shape, dtype=F32):
    return jax.ShapeDtypeStruct(shape, dtype)


def call_kdf(pos, base, code8, own8, p8, masks):
    return pl.pallas_call(
        kdf_kernel,
        out_shape=(shaped((128, 128)), shaped((3, 6, 6, 2, 128)), shaped((8, 8, 128))),
        in_specs=[VM] * 6, out_specs=(VM,) * 3,
        scratch_shapes=[pltpu.VMEM((10, 10, 32, 128), F32), pltpu.VMEM((10, 10, 32, 128), BF16), pltpu.VMEM((94, 128, 64), BF16),
                        pltpu.VMEM((8, 8, 128), F32), pltpu.VMEM((3, 8, 8, 128), F32), pltpu.VMEM((40, 112, 128), BF16),
                        pltpu.VMEM((162, 128, 256), F32)],
        compiler_params=pltpu.CompilerParams(vmem_limit_bytes=40 * 1024 * 1024),
        cost_estimate=pl.CostEstimate(flops=40_000_000, bytes_accessed=400_000, transcendentals=0),
        name="sweep")(pos, base, code8, own8, p8, masks)


def call_kc(seen, sums, code8, p8, gain):
    return pl.pallas_call(
        kc_kernel,
        out_shape=(shaped((10, 10, 2, 128)), shaped((8, 8, 128)), shaped((1, 128))),
        in_specs=[VM] * 5, out_specs=(VM,) * 3,
        compiler_params=pltpu.CompilerParams(vmem_limit_bytes=8 * 1024 * 1024),
        cost_estimate=pl.CostEstimate(flops=1_000_000, bytes_accessed=400_000, transcendentals=0),
        name="combine")(seen.reshape(128, 128), sums, code8, p8, gain)


FAR = 2.0 ** 20
TILES = [(gx, gy) for gx in range(8) for gy in range(16)]


def home_of(gx, gy):
    return gx * 16 + gy


def work_of(gx, gy):
    x = gx >> 1
    flip = (gx ^ x) & 1
    chip = gy >> 1
    high = chip >> 2
    y = chip & 3 if high == 0 else 3 - (chip & 3)
    return ((x * 2 + (flip ^ high)) * 2 + high) * 8 + y * 2 + ((gx + gy) & 1)


def to_work(block):
    return lax.ppermute(block, ALL, [(home_of(gx, gy), work_of(gx, gy)) for gx, gy in TILES])


def to_home(block):
    return lax.ppermute(block, ALL, [(work_of(gx, gy), home_of(gx, gy)) for gx, gy in TILES])


def partners(dim, near):
    pairs = []
    for gx, gy in TILES:
        place, count = ((gx, 8), (gy, 16))[dim]
        other = (place + (1 if (place % 2 == 0) == near else -1)) % count
        pairs.append((work_of(gx, gy), work_of(*((other, gy) if dim == 0 else (gx, other)))))
    return pairs


def swapped(block, even, dim):
    first = lax.slice_in_dim(block, 0, 2, axis=dim + 1)
    last = lax.slice_in_dim(block, 4, 6, axis=dim + 1)
    far = lax.ppermute(jnp.where(even, first, last), ALL, partners(dim, False))
    near = lax.ppermute(jnp.where(even, last, first), ALL, partners(dim, True))
    low = jnp.where(even, far, near)
    high = jnp.where(even, near, far)
    return jnp.concatenate([low, block, high], axis=dim + 1)


def padded(block):
    odd_x = lax.axis_index("gx_0") + lax.axis_index("gx_1") + lax.axis_index("gy_0")
    odd_y = odd_x + lax.axis_index("gy_2")
    return swapped(swapped(block, odd_x % 2 == 0, 0), odd_y % 2 == 0, 1)


def local(position, velocity, other_accel, phase_ids, counts):
    slot_index = jnp.arange(128, dtype=jnp.int32)
    live = slot_index[None, None, :] < counts[:, :, None]
    code = jnp.where(live, phase_ids + 1, 0).astype(F32)
    masks = jnp.asarray(offset_masks(), BF16)
    rest = position - 0.5 + TIME_STEP * (velocity + TIME_STEP * other_accel)
    base = jnp.stack([jnp.where(live, rest[0], FAR), jnp.where(live, rest[1], 0.0)], axis=2)
    packed = to_work(jnp.concatenate([base, code[:, :, None, :]], axis=2))
    base = packed[:, :, :2]
    first = padded(packed[None])[0]
    near = first[:, :, :2]
    code8 = first[1:9, 1:9, 2]
    own8 = jnp.pad(packed[:, :, 2], ((1, 1), (1, 1), (0, 0)))
    pressure = jnp.zeros((8, 8, 128), F32)
    rows = []
    for iteration in range(ITERS):
        last = iteration == ITERS - 1
        bounds, sums, gain = call_kdf(near, jnp.zeros_like(base) if last else base, code8, own8, pressure, masks)
        seen = lax.all_to_all(bounds, ALL, 0, 0, tiled=True)
        if not last:
            wide = padded(sums)
            near, pressure, row = call_kc(seen, wide, code8, pressure, gain)
            rows.append(row[0, :4])
    top = seen.reshape(128, 128).max(axis=0)
    row = jnp.concatenate([top[:2], -top[2:4]])
    rows.append(row)
    relax = 1.0 / (1.0 + row[:2] - row[2:])
    parts = jnp.stack([sums[0, :, :, 0], sums[0, :, :, 1], sums[1, :, :, 0], sums[1, :, :, 1], sums[2, :, :, 0], sums[2, :, :, 1],
                       pressure[1:7, 1:7], gain[1:7, 1:7]])
    parts = to_home(parts)
    delta = parts[0:2] + relax[0] * parts[2:4] + relax[1] * parts[4:6]
    new_velocity = jnp.where(live, velocity + TIME_STEP * other_accel + delta * (1.0 / TIME_STEP), 0.0)
    new_position = jnp.where(live, position + TIME_STEP * new_velocity, 0.0)
    new_pressure = parts[6] + jnp.where(phase_ids == 1, relax[1], relax[0]) * parts[7]
    return new_position, new_velocity, new_pressure, jnp.stack(rows)


def solution(mesh):
    torus = Mesh(mesh.devices.reshape(4, 2, 2, 4, 2), ("gx_0", "gx_1", "gy_0", "gy_1", "gy_2"))
    in_specs = (
        P(None, GX, GY, None),
        P(None, GX, GY, None),
        P(None, GX, GY, None),
        P(GX, GY, None),
        P(GX, GY),
    )
    out_specs = (P(None, GX, GY, None), P(None, GX, GY, None), P(GX, GY, None), P())
    return jax.shard_map(local, mesh=torus, in_specs=in_specs, out_specs=out_specs, check_vma=False)
```

```python
import jax
import jax.numpy as jnp
import numpy as np
from jax import lax
from jax.experimental import pallas as pl
from jax.experimental.pallas import tpu as pltpu
from jax.sharding import Mesh
from jax.sharding import PartitionSpec as P

ITERS = 4
GX = ("gx_0", "gx_1")
GY = ("gy_0", "gy_1", "gy_2")
ALL = GX + GY

F32, BF16 = jnp.float32, jnp.bfloat16
OFFS = tuple((ox, oy) for ox in (-1, 0, 1) for oy in (-1, 0, 1))


def offset_masks():
    out = np.ones((9, 32, 128), np.float32)
    for k, (ox, oy) in enumerate(OFFS):
        for row in (6, 7, 12, 13, 14, 15, 18, 19, 20, 21, 22, 23):
            out[k, row] = (ox, oy)[row % 2]
        out[k, 31] = ox * ox + oy * oy
    return out


def rnd(v):
    return v.astype(BF16).astype(F32)


def row_iota():
    return lax.broadcasted_iota(jnp.int32, (8, 128), 0)


def cell_slabs(pos_ref, r, c, want_l=True, want_r=True):
    row = row_iota()
    x = jnp.broadcast_to(pos_ref[r, c, 0:1, :], (8, 128))
    y = jnp.broadcast_to(pos_ref[r, c, 1:2, :], (8, 128))
    v = jnp.where((row & 1) == 1, y, x)
    v1 = rnd(v)
    rest = v - v1
    v2 = rnd(rest)
    v3 = rest - v2
    n = x * x + y * y
    n1 = rnd(n)
    nrest = n - n1
    n2 = rnd(nrest)
    n3 = nrest - n2
    left = right = None
    if want_l:
        la = v1
        lb = jnp.where((row == 4) | (row == 5), 1.0, v2)
        lc = jnp.where((row >= 2) & (row <= 5), 1.0, v3)
        ld = jnp.where(row == 0, n1, jnp.where(row == 1, n2, jnp.where(row == 2, n3, 1.0)))
        left = jnp.concatenate([la, lb, lc, ld], axis=0)
    if want_r:
        t1, t2, t3 = 2.0 * v1, 2.0 * v2, 2.0 * v3
        ra = jnp.where(row < 2, t1, jnp.where(row < 4, t2, jnp.where(row < 6, t3, -2.0)))
        rb = ra
        rc = jnp.where(row < 4, t1, jnp.where(row < 6, t2, -2.0))
        rd = jnp.where(row < 3, -1.0, jnp.where(row == 3, -n1, jnp.where(row == 4, -n2, jnp.where(row == 5, -n3, jnp.where(row == 6, 1.0, -1.0)))))
        right = jnp.concatenate([ra, rb, rc, rd], axis=0)
    return left, right


def pair_rhs(r1, r2, mask):
    zero = jnp.zeros((32, 128), BF16)
    return jnp.concatenate(
        [jnp.concatenate([r1 * mask, zero], axis=1), jnp.concatenate([zero, r2 * mask], axis=1)], axis=0)


def pair_s(left_t, rhs):
    return jnp.dot(left_t, rhs, preferred_element_type=F32)


def fill_slabs(pos_ref, ls, rs, lo, hi, rlo, rhi):
    def body(r, carry):
        for c in range(lo, hi):
            left, right = cell_slabs(pos_ref, r, c, True, rlo <= c < rhi)
            ls[r, c] = left
            if rlo <= c < rhi:
                rs[r, c] = right.astype(BF16)
        return carry
    lax.fori_loop(lo, hi, body, 0)


def fill_pairs(ls, lt, start, rows, cols, dr, dc, rbase, cbase):
    for i in range(rows):
        for j in range(cols):
            both = jnp.concatenate([ls[rbase + i, cbase + j], ls[rbase + i + dr, cbase + j + dc]], axis=0)
            lt[start + i * cols + j] = both.T.astype(BF16)


def density_pair(rs, lt, masks_ref, i1, i2, first, stride, squares=None, at=0):
    r1, r2 = rs[i1[0], i1[1]], rs[i2[0], i2[1]]
    acc = jnp.zeros((8, 256), F32)
    for k, (ox, oy) in enumerate(OFFS):
        s = pair_s(lt[first + ox * stride + oy], pair_rhs(r1, r2, masks_ref[k]))
        w = jnp.maximum(s, 0.0)
        w2 = w * w
        if squares is not None:
            squares[at * 9 + k] = w2
        w3 = w2 * w
        acc = acc + w3.reshape(16, 8, 256).sum(axis=0)
    return acc.sum(axis=0, keepdims=True)


OWN, TB, LR, FP = 9, 8, 6, 6
TIME_STEP = 0.05
KERNEL_NORM = 4.0 / (3.141592653589793 * 64.0)
SENTINEL = 1.0e30


def bounds_of(dens, code, bnd_ref):
    ratio = dens * jnp.where(code == 2.0, KERNEL_NORM / 1.5, KERNEL_NORM / 1.2)
    picks = []
    for phase in (1.0, 2.0):
        picks.append(jnp.where(code == phase, ratio, -SENTINEL))
    for phase in (1.0, 2.0):
        picks.append(jnp.where(code == phase, -ratio, -SENTINEL))
    lane = lax.broadcasted_iota(jnp.int32, (1, 128), 1)
    out = jnp.zeros((1, 128), F32)
    for k, pick in enumerate(picks):
        top = pick.max(axis=0).max(axis=0, keepdims=True).max(axis=1, keepdims=True)
        out = jnp.where(lane == k, top, out)
    bnd_ref[...] = jnp.broadcast_to(out, (128, 128))


def term_rows(t_ref, r, c):
    row = row_iota() & 3
    a, b0, b1 = (jnp.broadcast_to(t_ref[k, r, pl.ds(c, 1), :], (8, 128)) for k in range(3))
    return jnp.where(row == 0, 1.0, jnp.where(row == 1, a, jnp.where(row == 2, b0, b1)))


def hi_lo(v):
    hi = rnd(v)
    return jnp.where(row_iota() < 4, hi, v - hi)


def cell_moments(pos_ref, t_ref, r, c):
    t = term_rows(t_ref, r, c)
    x = jnp.broadcast_to(pos_ref[r + 1, c + 1, 0:1, :], (8, 128))
    y = jnp.broadcast_to(pos_ref[r + 1, c + 1, 1:2, :], (8, 128))
    groups = [hi_lo(t)]
    for q in (x, y):
        for o in (-1.0, 0.0, 1.0):
            groups.append(hi_lo(t * (q + o)))
    return groups


def kdf_kernel(pos_ref, base_ref, code_ref, own_ref, p_ref, masks_ref, bnd_ref, s_ref, q_ref, ls, rs, lt, dn, tt, gt, squares):
    fill_slabs(pos_ref, ls, rs, 0, 10, 1, 9)
    fill_pairs(ls, lt, 0, 5, 8, 3, 0, 1, 1)
    fill_pairs(ls, lt, 40, 3, 10, 7, 0, 0, 0)
    fill_pairs(ls, lt, 70, 8, 3, 0, 7, 1, 0)
    def own(step, carry):
        for u in range(OWN):
            n = step * OWN + u
            a, b = (u % 3, step * (OWN // 3) + u // 3) if OWN % 3 == 0 else (n % 3, n // 3)
            row = density_pair(rs, lt, masks_ref, (a + 2, b + 2), (a + 5, b + 2), (a + 1) * 8 + b + 1, 8, squares, n)
            dn[a + 1, pl.ds(b + 1, 1), :] = row[:, :128]
            dn[a + 4, pl.ds(b + 1, 1), :] = row[:, 128:]
        return carry
    lax.fori_loop(0, 18 // OWN, own, 0)
    def top_bottom(h, carry):
        for u in range(TB):
            c = h * TB + u
            row = density_pair(rs, lt, masks_ref, (1, c + 1), (8, c + 1), 50 + c + 1, 10)
            dn[0, pl.ds(c, 1), :] = row[:, :128]
            dn[7, pl.ds(c, 1), :] = row[:, 128:]
        return carry
    lax.fori_loop(0, 8 // TB, top_bottom, 0)
    def left_right(h, carry):
        for u in range(LR):
            a = h * LR + u + 1
            row = density_pair(rs, lt, masks_ref, (a + 1, 1), (a + 1, 8), 70 + a * 3 + 1, 3)
            dn[a, pl.ds(0, 1), :] = row[:, :128]
            dn[a, pl.ds(7, 1), :] = row[:, 128:]
        return carry
    lax.fori_loop(0, 6 // LR, left_right, 0)
    bounds_of(dn[...], own_ref[...], bnd_ref)
    code = code_ref[...]
    live = code > 0.0
    heavy = code == 2.0
    density = KERNEL_NORM * dn[...]
    ratio = density * jnp.where(heavy, 1.0 / 1.5, 1.0 / 1.2)
    q = jnp.where(live, jnp.where(heavy, 200.0, 100.0) * (ratio - 1.0), 0.0)
    q_ref[...] = q
    safe = jnp.where(live, density, 1.0)
    inv = jnp.where(live, 1.0 / (safe * safe), 0.0)
    b = q * inv
    tt[0] = p_ref[...] * inv
    tt[1] = jnp.where(heavy, 0.0, b)
    tt[2] = jnp.where(heavy, b, 0.0)
    def moments(i, carry):
        for j in range(8):
            one = cell_moments(pos_ref, tt, i, j)
            two = cell_moments(pos_ref, tt, i + 3, j)
            tiles = [jnp.concatenate([g, h], axis=0) for g, h in zip(one, two)]
            gt[i * 8 + j] = jnp.concatenate(tiles, axis=0).astype(BF16)
        return carry
    lax.fori_loop(0, 5, moments, 0)
    row = row_iota()
    def forces(step, carry):
        accs = [jnp.zeros((48, 256), F32) for _ in range(FP)]
        work = [((FP * step + m) % 3, (FP * step + m) // 3) for m in range(FP)]
        for k, (ox, oy) in enumerate(OFFS):
            for m in range(FP):
                a, bcol = work[m]
                p = (a + 1 + ox) * 8 + bcol + 1 + oy
                w2 = squares[(FP * step + m) * 9 + k]
                hi = w2.astype(BF16)
                lo = (w2 - hi.astype(F32)).astype(BF16)
                g = jnp.concatenate([gt[p, 0:16], gt[p, 32 + 16 * ox:48 + 16 * ox], gt[p, 80 + 16 * oy:96 + 16 * oy]], axis=0)
                accs[m] = accs[m] + jnp.dot(jnp.concatenate([g, g], axis=1), jnp.concatenate([hi, lo], axis=0), preferred_element_type=F32)
        for m in range(FP):
            a, bcol = work[m]
            acc = accs[m]
            for h in range(2):
                aa = a + 3 * h
                lanes = slice(128 * h, 128 * h + 128)
                sums = []
                for t in range(3):
                    m = acc[16 * t + 8 * h:16 * t + 8 * h + 8, lanes]
                    sums.append(m + jnp.concatenate([m[4:8], m[0:4]], axis=0))
                x = jnp.broadcast_to(pos_ref[aa + 2, bcol + 2, 0:1, :], (8, 128))
                y = jnp.broadcast_to(pos_ref[aa + 2, bcol + 2, 1:2, :], (8, 128))
                ex = x * sums[0] - sums[1]
                ey = y * sums[0] - sums[2]
                e = jnp.where(row < 4, ex, ey)
                e0 = jnp.where(row < 4, jnp.broadcast_to(ex[0:1], (8, 128)), jnp.broadcast_to(ey[0:1], (8, 128)))
                code_row = jnp.broadcast_to(code_ref[aa + 1, pl.ds(bcol + 1, 1), :], (8, 128))
                scale = 6.0 * KERNEL_NORM * TIME_STEP * TIME_STEP
                coef = jnp.where(code_row == 2.0, scale / 1.5, jnp.where(code_row == 1.0, scale, 0.0))
                out = coef * (term_rows(tt, aa + 1, bcol + 1) * e0 + e)
                s_ref[0, aa, bcol, 0:1, :] = base_ref[aa, bcol, 0:1, :] + out[1:2]
                s_ref[0, aa, bcol, 1:2, :] = base_ref[aa, bcol, 1:2, :] + out[5:6]
                for t in (1, 2):
                    s_ref[t, aa, bcol, 0:1, :] = out[t + 1:t + 2]
                    s_ref[t, aa, bcol, 1:2, :] = out[t + 5:t + 6]
        return carry
    lax.fori_loop(0, 18 // FP, forces, 0)


def kc_kernel(seen_ref, s_ref, code_ref, p_ref, q_ref, pos_ref, pout_ref, row_ref):
    top = seen_ref[...].max(axis=0, keepdims=True)
    lane = lax.broadcasted_iota(jnp.int32, (1, 128), 1)
    top0, top1, neg0, neg1 = (jnp.sum(jnp.where(lane == k, top, 0.0), axis=1, keepdims=True) for k in range(4))
    r0 = 1.0 / (1.0 + top0 + neg0)
    r1 = 1.0 / (1.0 + top1 + neg1)
    row_ref[...] = jnp.where(lane < 2, top, jnp.where(lane < 4, -top, jnp.where(lane == 4, r0, r1)))
    for a in range(8):
        pout_ref[a] = p_ref[a] + jnp.where(code_ref[a] == 2.0, r1, r0) * q_ref[a]
    for a in range(10):
        pos_ref[a] = s_ref[0, a] + r0[None] * s_ref[1, a] + r1[None] * s_ref[2, a]


VM = pl.BlockSpec(memory_space=pltpu.VMEM)


def shaped(shape, dtype=F32):
    return jax.ShapeDtypeStruct(shape, dtype)


def call_kdf(pos, base, code8, own8, p8, masks):
    return pl.pallas_call(
        kdf_kernel,
        out_shape=(shaped((128, 128)), shaped((3, 6, 6, 2, 128)), shaped((8, 8, 128))),
        in_specs=[VM] * 6, out_specs=(VM,) * 3,
        scratch_shapes=[pltpu.VMEM((10, 10, 32, 128), F32), pltpu.VMEM((10, 10, 32, 128), BF16), pltpu.VMEM((94, 128, 64), BF16),
                        pltpu.VMEM((8, 8, 128), F32), pltpu.VMEM((3, 8, 8, 128), F32), pltpu.VMEM((40, 112, 128), BF16),
                        pltpu.VMEM((162, 128, 256), F32)],
        compiler_params=pltpu.CompilerParams(vmem_limit_bytes=40 * 1024 * 1024),
        cost_estimate=pl.CostEstimate(flops=40_000_000, bytes_accessed=400_000, transcendentals=0),
        name="sweep")(pos, base, code8, own8, p8, masks)


def call_kc(seen, sums, code8, p8, gain):
    return pl.pallas_call(
        kc_kernel,
        out_shape=(shaped((10, 10, 2, 128)), shaped((8, 8, 128)), shaped((1, 128))),
        in_specs=[VM] * 5, out_specs=(VM,) * 3,
        compiler_params=pltpu.CompilerParams(vmem_limit_bytes=8 * 1024 * 1024),
        cost_estimate=pl.CostEstimate(flops=1_000_000, bytes_accessed=400_000, transcendentals=0),
        name="combine")(seen.reshape(128, 128), sums, code8, p8, gain)


FAR = 2.0 ** 20
TILES = [(gx, gy) for gx in range(8) for gy in range(16)]


def home_of(gx, gy):
    return gx * 16 + gy


def work_of(gx, gy):
    x = gx >> 1
    flip = (gx ^ x) & 1
    chip = gy >> 1
    high = chip >> 2
    y = chip & 3 if high == 0 else 3 - (chip & 3)
    return ((x * 2 + (flip ^ high)) * 2 + high) * 8 + y * 2 + ((gx + gy) & 1)


def to_work(block):
    return lax.ppermute(block, ALL, [(home_of(gx, gy), work_of(gx, gy)) for gx, gy in TILES])


def to_home(block):
    return lax.ppermute(block, ALL, [(work_of(gx, gy), home_of(gx, gy)) for gx, gy in TILES])


def partners(dim, near):
    pairs = []
    for gx, gy in TILES:
        place, count = ((gx, 8), (gy, 16))[dim]
        other = (place + (1 if (place % 2 == 0) == near else -1)) % count
        pairs.append((work_of(gx, gy), work_of(*((other, gy) if dim == 0 else (gx, other)))))
    return pairs


def swapped(block, even, dim):
    first = lax.slice_in_dim(block, 0, 2, axis=dim + 1)
    last = lax.slice_in_dim(block, 4, 6, axis=dim + 1)
    far = lax.ppermute(jnp.where(even, first, last), ALL, partners(dim, False))
    near = lax.ppermute(jnp.where(even, last, first), ALL, partners(dim, True))
    low = jnp.where(even, far, near)
    high = jnp.where(even, near, far)
    return jnp.concatenate([low, block, high], axis=dim + 1)


def padded(block):
    odd_x = lax.axis_index("gx_0") + lax.axis_index("gx_1") + lax.axis_index("gy_0")
    odd_y = odd_x + lax.axis_index("gy_2")
    block = swapped(block, odd_x % 2 == 0, 0)
    return swapped(block, odd_y % 2 == 0, 1)


def local(position, velocity, other_accel, phase_ids, counts):
    slot_index = jnp.arange(128, dtype=jnp.int32)
    live = slot_index[None, None, :] < counts[:, :, None]
    code = jnp.where(live, phase_ids + 1, 0).astype(F32)
    masks = jnp.asarray(offset_masks(), BF16)
    rest = position - 0.5 + TIME_STEP * (velocity + TIME_STEP * other_accel)
    base = jnp.stack([jnp.where(live, rest[0], FAR), jnp.where(live, rest[1], 0.0)], axis=2)
    packed = to_work(jnp.concatenate([base, code[:, :, None, :]], axis=2))
    base = packed[:, :, :2]
    first = padded(packed[None])[0]
    near = first[:, :, :2]
    code8 = first[1:9, 1:9, 2]
    own8 = jnp.pad(packed[:, :, 2], ((1, 1), (1, 1), (0, 0)))
    pressure = jnp.zeros((8, 8, 128), F32)
    rows = []
    for iteration in range(ITERS):
        last = iteration == ITERS - 1
        bounds, sums, gain = call_kdf(near, jnp.zeros_like(base) if last else base, code8, own8, pressure, masks)
        seen = lax.all_to_all(bounds, ALL, 0, 0, tiled=True)
        if not last:
            wide = padded(sums)
            near, pressure, row = call_kc(seen, wide, code8, pressure, gain)
            rows.append(row[0, :4])
    top = seen.reshape(128, 128).max(axis=0)
    row = jnp.concatenate([top[:2], -top[2:4]])
    rows.append(row)
    relax = 1.0 / (1.0 + row[:2] - row[2:])
    parts = jnp.stack([sums[0, :, :, 0], sums[0, :, :, 1], sums[1, :, :, 0], sums[1, :, :, 1], sums[2, :, :, 0], sums[2, :, :, 1],
                       pressure[1:7, 1:7], gain[1:7, 1:7]])
    parts = to_home(parts)
    delta = parts[0:2] + relax[0] * parts[2:4] + relax[1] * parts[4:6]
    new_velocity = jnp.where(live, velocity + TIME_STEP * other_accel + delta * (1.0 / TIME_STEP), 0.0)
    new_position = jnp.where(live, position + TIME_STEP * new_velocity, 0.0)
    new_pressure = parts[6] + jnp.where(phase_ids == 1, relax[1], relax[0]) * parts[7]
    return new_position, new_velocity, new_pressure, jnp.stack(rows)


def solution(mesh):
    torus = Mesh(mesh.devices.reshape(4, 2, 2, 4, 2), ("gx_0", "gx_1", "gy_0", "gy_1", "gy_2"))
    in_specs = (
        P(None, GX, GY, None),
        P(None, GX, GY, None),
        P(None, GX, GY, None),
        P(GX, GY, None),
        P(GX, GY),
    )
    out_specs = (P(None, GX, GY, None), P(None, GX, GY, None), P(GX, GY, None), P())
    return jax.shard_map(local, mesh=torus, in_specs=in_specs, out_specs=out_specs, check_vma=False)
```

```python
import jax
import jax.numpy as jnp
import numpy as np
from jax import lax
from jax.experimental import pallas as pl
from jax.experimental.pallas import tpu as pltpu
from jax.sharding import Mesh
from jax.sharding import PartitionSpec as P

ITERS = 4
GX = ("gx_0", "gx_1")
GY = ("gy_0", "gy_1", "gy_2")
ALL = GX + GY

F32, BF16 = jnp.float32, jnp.bfloat16
OFFS = tuple((ox, oy) for ox in (-1, 0, 1) for oy in (-1, 0, 1))


def offset_masks():
    out = np.ones((9, 32, 128), np.float32)
    for k, (ox, oy) in enumerate(OFFS):
        for row in (6, 7, 12, 13, 14, 15, 18, 19, 20, 21, 22, 23):
            out[k, row] = (ox, oy)[row % 2]
        out[k, 31] = ox * ox + oy * oy
    return out


def rnd(v):
    return v.astype(BF16).astype(F32)


def row_iota():
    return lax.broadcasted_iota(jnp.int32, (8, 128), 0)


def cell_slabs(pos_ref, r, c, want_l=True, want_r=True):
    row = row_iota()
    x = jnp.broadcast_to(pos_ref[r, c, 0:1, :], (8, 128))
    y = jnp.broadcast_to(pos_ref[r, c, 1:2, :], (8, 128))
    v = jnp.where((row & 1) == 1, y, x)
    v1 = rnd(v)
    rest = v - v1
    v2 = rnd(rest)
    v3 = rest - v2
    n = x * x + y * y
    n1 = rnd(n)
    nrest = n - n1
    n2 = rnd(nrest)
    n3 = nrest - n2
    left = right = None
    if want_l:
        la = v1
        lb = jnp.where((row == 4) | (row == 5), 1.0, v2)
        lc = jnp.where((row >= 2) & (row <= 5), 1.0, v3)
        ld = jnp.where(row == 0, n1, jnp.where(row == 1, n2, jnp.where(row == 2, n3, 1.0)))
        left = jnp.concatenate([la, lb, lc, ld], axis=0)
    if want_r:
        t1, t2, t3 = 2.0 * v1, 2.0 * v2, 2.0 * v3
        ra = jnp.where(row < 2, t1, jnp.where(row < 4, t2, jnp.where(row < 6, t3, -2.0)))
        rb = ra
        rc = jnp.where(row < 4, t1, jnp.where(row < 6, t2, -2.0))
        rd = jnp.where(row < 3, -1.0, jnp.where(row == 3, -n1, jnp.where(row == 4, -n2, jnp.where(row == 5, -n3, jnp.where(row == 6, 1.0, -1.0)))))
        right = jnp.concatenate([ra, rb, rc, rd], axis=0)
    return left, right


def pair_rhs(r1, r2, mask):
    zero = jnp.zeros((32, 128), BF16)
    return jnp.concatenate(
        [jnp.concatenate([r1 * mask, zero], axis=1), jnp.concatenate([zero, r2 * mask], axis=1)], axis=0)


def pair_s(left_t, rhs):
    return jnp.dot(left_t, rhs, preferred_element_type=F32)


def fill_slabs(pos_ref, ls, rs, lo, hi, rlo, rhi):
    def body(r, carry):
        for c in range(lo, hi):
            left, right = cell_slabs(pos_ref, r, c, True, rlo <= c < rhi)
            ls[r, c] = left
            if rlo <= c < rhi:
                rs[r, c] = right.astype(BF16)
        return carry
    lax.fori_loop(lo, hi, body, 0)


def fill_pairs(ls, lt, start, rows, cols, dr, dc, rbase, cbase):
    for i in range(rows):
        for j in range(cols):
            both = jnp.concatenate([ls[rbase + i, cbase + j], ls[rbase + i + dr, cbase + j + dc]], axis=0)
            lt[start + i * cols + j] = both.T.astype(BF16)


def density_pair(rs, lt, masks_ref, i1, i2, first, stride, squares=None, at=0):
    r1, r2 = rs[i1[0], i1[1]], rs[i2[0], i2[1]]
    acc = jnp.zeros((8, 256), F32)
    for k, (ox, oy) in enumerate(OFFS):
        s = pair_s(lt[first + ox * stride + oy], pair_rhs(r1, r2, masks_ref[k]))
        w = jnp.maximum(s, 0.0)
        w2 = w * w
        if squares is not None:
            squares[at * 9 + k] = w2
        w3 = w2 * w
        acc = acc + w3.reshape(16, 8, 256).sum(axis=0)
    return acc.sum(axis=0, keepdims=True)


OWN, RING, FP = 9, 7, 6
TIME_STEP = 0.05
KERNEL_NORM = 4.0 / (3.141592653589793 * 64.0)
SENTINEL = 1.0e30


def bounds_of(dens, code, bnd_ref):
    ratio = dens * jnp.where(code == 2.0, KERNEL_NORM / 1.5, KERNEL_NORM / 1.2)
    picks = []
    for phase in (1.0, 2.0):
        picks.append(jnp.where(code == phase, ratio, -SENTINEL))
    for phase in (1.0, 2.0):
        picks.append(jnp.where(code == phase, -ratio, -SENTINEL))
    lane = lax.broadcasted_iota(jnp.int32, (1, 128), 1)
    out = jnp.zeros((1, 128), F32)
    for k, pick in enumerate(picks):
        top = pick.max(axis=0).max(axis=0, keepdims=True).max(axis=1, keepdims=True)
        out = jnp.where(lane == k, top, out)
    bnd_ref[...] = jnp.broadcast_to(out, (128, 128))


def term_rows(t_ref, r, c):
    row = row_iota() & 3
    a, b0, b1 = (jnp.broadcast_to(t_ref[k, r, pl.ds(c, 1), :], (8, 128)) for k in range(3))
    return jnp.where(row == 0, 1.0, jnp.where(row == 1, a, jnp.where(row == 2, b0, b1)))


def hi_lo(v):
    hi = rnd(v)
    return jnp.where(row_iota() < 4, hi, v - hi)


def cell_moments(pos_ref, t_ref, r, c):
    t = term_rows(t_ref, r, c)
    x = jnp.broadcast_to(pos_ref[r + 1, c + 1, 0:1, :], (8, 128))
    y = jnp.broadcast_to(pos_ref[r + 1, c + 1, 1:2, :], (8, 128))
    groups = [hi_lo(t)]
    for q in (x, y):
        for o in (-1.0, 0.0, 1.0):
            groups.append(hi_lo(t * (q + o)))
    return groups


def kdf_kernel(pos_ref, base_ref, code_ref, own_ref, p_ref, masks_ref, bnd_ref, s_ref, q_ref, ls, rs, lt, dn, tt, gt, squares):
    fill_slabs(pos_ref, ls, rs, 0, 10, 1, 9)
    fill_pairs(ls, lt, 0, 5, 8, 3, 0, 1, 1)
    fill_pairs(ls, lt, 40, 3, 10, 7, 0, 0, 0)
    fill_pairs(ls, lt, 70, 8, 3, 0, 7, 1, 0)
    def own(step, carry):
        for u in range(OWN):
            n = step * OWN + u
            a, b = (u % 3, step * (OWN // 3) + u // 3) if OWN % 3 == 0 else (n % 3, n // 3)
            row = density_pair(rs, lt, masks_ref, (a + 2, b + 2), (a + 5, b + 2), (a + 1) * 8 + b + 1, 8, squares, n)
            dn[a + 1, pl.ds(b + 1, 1), :] = row[:, :128]
            dn[a + 4, pl.ds(b + 1, 1), :] = row[:, 128:]
        return carry
    lax.fori_loop(0, 18 // OWN, own, 0)
    def ring(step, carry):
        for u in range(RING):
            n = step * RING + u
            flat = n < 8
            r1, r2, c1, c2 = (jnp.where(flat, p, q) for p, q in ((1, n - 6), (8, n - 6), (n + 1, 1), (n + 1, 8)))
            row = density_pair(rs, lt, masks_ref, (r1, c1), (r2, c2), jnp.where(flat, n + 51, 3 * n + 50), jnp.where(flat, 10, 3))
            dn[r1 - 1, pl.ds(c1 - 1, 1), :] = row[:, :128]
            dn[r2 - 1, pl.ds(c2 - 1, 1), :] = row[:, 128:]
        return carry
    lax.fori_loop(0, 14 // RING, ring, 0)
    bounds_of(dn[...], own_ref[...], bnd_ref)
    code = code_ref[...]
    live = code > 0.0
    heavy = code == 2.0
    density = KERNEL_NORM * dn[...]
    ratio = density * jnp.where(heavy, 1.0 / 1.5, 1.0 / 1.2)
    q = jnp.where(live, jnp.where(heavy, 200.0, 100.0) * (ratio - 1.0), 0.0)
    q_ref[...] = q
    safe = jnp.where(live, density, 1.0)
    inv = jnp.where(live, 1.0 / (safe * safe), 0.0)
    b = q * inv
    tt[0] = p_ref[...] * inv
    tt[1] = jnp.where(heavy, 0.0, b)
    tt[2] = jnp.where(heavy, b, 0.0)
    def moments(i, carry):
        for j in range(8):
            one = cell_moments(pos_ref, tt, i, j)
            two = cell_moments(pos_ref, tt, i + 3, j)
            tiles = [jnp.concatenate([g, h], axis=0) for g, h in zip(one, two)]
            gt[i * 8 + j] = jnp.concatenate(tiles, axis=0).astype(BF16)
        return carry
    lax.fori_loop(0, 5, moments, 0)
    row = row_iota()
    def forces(step, carry):
        accs = [jnp.zeros((48, 256), F32) for _ in range(FP)]
        work = [((FP * step + m) % 3, (FP * step + m) // 3) for m in range(FP)]
        for k, (ox, oy) in enumerate(OFFS):
            for m in range(FP):
                a, bcol = work[m]
                p = (a + 1 + ox) * 8 + bcol + 1 + oy
                w2 = squares[(FP * step + m) * 9 + k]
                hi = w2.astype(BF16)
                lo = (w2 - hi.astype(F32)).astype(BF16)
                g = jnp.concatenate([gt[p, 0:16], gt[p, 32 + 16 * ox:48 + 16 * ox], gt[p, 80 + 16 * oy:96 + 16 * oy]], axis=0)
                accs[m] = accs[m] + jnp.dot(jnp.concatenate([g, g], axis=1), jnp.concatenate([hi, lo], axis=0), preferred_element_type=F32)
        for m in range(FP):
            a, bcol = work[m]
            acc = accs[m]
            for h in range(2):
                aa = a + 3 * h
                lanes = slice(128 * h, 128 * h + 128)
                sums = []
                for t in range(3):
                    m = acc[16 * t + 8 * h:16 * t + 8 * h + 8, lanes]
                    sums.append(m + jnp.concatenate([m[4:8], m[0:4]], axis=0))
                x = jnp.broadcast_to(pos_ref[aa + 2, bcol + 2, 0:1, :], (8, 128))
                y = jnp.broadcast_to(pos_ref[aa + 2, bcol + 2, 1:2, :], (8, 128))
                ex = x * sums[0] - sums[1]
                ey = y * sums[0] - sums[2]
                e = jnp.where(row < 4, ex, ey)
                e0 = jnp.where(row < 4, jnp.broadcast_to(ex[0:1], (8, 128)), jnp.broadcast_to(ey[0:1], (8, 128)))
                code_row = jnp.broadcast_to(code_ref[aa + 1, pl.ds(bcol + 1, 1), :], (8, 128))
                scale = 6.0 * KERNEL_NORM * TIME_STEP * TIME_STEP
                coef = jnp.where(code_row == 2.0, scale / 1.5, jnp.where(code_row == 1.0, scale, 0.0))
                out = coef * (term_rows(tt, aa + 1, bcol + 1) * e0 + e)
                s_ref[0, aa, bcol, 0:1, :] = base_ref[aa, bcol, 0:1, :] + out[1:2]
                s_ref[0, aa, bcol, 1:2, :] = base_ref[aa, bcol, 1:2, :] + out[5:6]
                for t in (1, 2):
                    s_ref[t, aa, bcol, 0:1, :] = out[t + 1:t + 2]
                    s_ref[t, aa, bcol, 1:2, :] = out[t + 5:t + 6]
        return carry
    lax.fori_loop(0, 18 // FP, forces, 0)


def kc_kernel(seen_ref, s_ref, code_ref, p_ref, q_ref, pos_ref, pout_ref, row_ref):
    top = seen_ref[...].max(axis=0, keepdims=True)
    lane = lax.broadcasted_iota(jnp.int32, (1, 128), 1)
    top0, top1, neg0, neg1 = (jnp.sum(jnp.where(lane == k, top, 0.0), axis=1, keepdims=True) for k in range(4))
    r0 = 1.0 / (1.0 + top0 + neg0)
    r1 = 1.0 / (1.0 + top1 + neg1)
    row_ref[...] = jnp.where(lane < 2, top, jnp.where(lane < 4, -top, jnp.where(lane == 4, r0, r1)))
    for a in range(8):
        pout_ref[a] = p_ref[a] + jnp.where(code_ref[a] == 2.0, r1, r0) * q_ref[a]
    for a in range(10):
        pos_ref[a] = s_ref[0, a] + r0[None] * s_ref[1, a] + r1[None] * s_ref[2, a]


VM = pl.BlockSpec(memory_space=pltpu.VMEM)


def shaped(shape, dtype=F32):
    return jax.ShapeDtypeStruct(shape, dtype)


def call_kdf(pos, base, code8, own8, p8, masks):
    return pl.pallas_call(
        kdf_kernel,
        out_shape=(shaped((128, 128)), shaped((3, 6, 6, 2, 128)), shaped((8, 8, 128))),
        in_specs=[VM] * 6, out_specs=(VM,) * 3,
        scratch_shapes=[pltpu.VMEM((10, 10, 32, 128), F32), pltpu.VMEM((10, 10, 32, 128), BF16), pltpu.VMEM((94, 128, 64), BF16),
                        pltpu.VMEM((8, 8, 128), F32), pltpu.VMEM((3, 8, 8, 128), F32), pltpu.VMEM((40, 112, 128), BF16),
                        pltpu.VMEM((162, 128, 256), F32)],
        compiler_params=pltpu.CompilerParams(vmem_limit_bytes=40 * 1024 * 1024),
        cost_estimate=pl.CostEstimate(flops=40_000_000, bytes_accessed=400_000, transcendentals=0),
        name="sweep")(pos, base, code8, own8, p8, masks)


def call_kc(seen, sums, code8, p8, gain):
    return pl.pallas_call(
        kc_kernel,
        out_shape=(shaped((10, 10, 2, 128)), shaped((8, 8, 128)), shaped((1, 128))),
        in_specs=[VM] * 5, out_specs=(VM,) * 3,
        compiler_params=pltpu.CompilerParams(vmem_limit_bytes=8 * 1024 * 1024),
        cost_estimate=pl.CostEstimate(flops=1_000_000, bytes_accessed=400_000, transcendentals=0),
        name="combine")(seen.reshape(128, 128), sums, code8, p8, gain)


def kz_kernel(seen_ref, parts_ref, pos_ref, vel_ref, acc_ref, code_ref, a_ref, b_ref, c_ref, npos_ref, nvel_ref, press_ref, mon_ref):
    top = seen_ref[...].max(axis=0, keepdims=True)
    lane = lax.broadcasted_iota(jnp.int32, (1, 128), 1)
    top0, top1, neg0, neg1 = (jnp.sum(jnp.where(lane == k, top, 0.0), axis=1, keepdims=True) for k in range(4))
    r0 = (1.0 / (1.0 + top0 + neg0))[None]
    r1 = (1.0 / (1.0 + top1 + neg1))[None]
    row = jnp.where(lane < 2, top, -top)
    mon_ref[...] = jnp.concatenate([a_ref[...], b_ref[...], c_ref[...], row], axis=0)[:, :4]
    code = code_ref[...]
    live = code > 0.0
    for c in range(2):
        delta = parts_ref[c] + r0 * parts_ref[2 + c] + r1 * parts_ref[4 + c]
        speed = jnp.where(live, vel_ref[c] + TIME_STEP * acc_ref[c] + delta * (1.0 / TIME_STEP), 0.0)
        nvel_ref[c] = speed
        npos_ref[c] = jnp.where(live, pos_ref[c] + TIME_STEP * speed, 0.0)
    press_ref[...] = parts_ref[6] + jnp.where(code == 2.0, r1, r0) * parts_ref[7]


def call_kz(seen, parts, position, velocity, other_accel, code, rows):
    return pl.pallas_call(
        kz_kernel,
        out_shape=(shaped((2, 6, 6, 128)), shaped((2, 6, 6, 128)), shaped((6, 6, 128)), shaped((4, 4))),
        in_specs=[VM] * 9, out_specs=(VM,) * 4,
        compiler_params=pltpu.CompilerParams(vmem_limit_bytes=8 * 1024 * 1024),
        cost_estimate=pl.CostEstimate(flops=1_000_000, bytes_accessed=400_000, transcendentals=0),
        name="finish")(seen.reshape(128, 128), parts, position, velocity, other_accel, code, *rows)


FAR = 2.0 ** 20
TILES = [(gx, gy) for gx in range(8) for gy in range(16)]


def home_of(gx, gy):
    return gx * 16 + gy


def work_of(gx, gy):
    x = gx >> 1
    flip = (gx ^ x) & 1
    chip = gy >> 1
    high = chip >> 2
    y = chip & 3 if high == 0 else 3 - (chip & 3)
    return ((x * 2 + (flip ^ high)) * 2 + high) * 8 + y * 2 + ((gx + gy) & 1)


def to_work(block):
    return lax.ppermute(block, ALL, [(home_of(gx, gy), work_of(gx, gy)) for gx, gy in TILES])


def to_home(block):
    return lax.ppermute(block, ALL, [(work_of(gx, gy), home_of(gx, gy)) for gx, gy in TILES])


def partners(dim, near):
    pairs = []
    for gx, gy in TILES:
        place, count = ((gx, 8), (gy, 16))[dim]
        other = (place + (1 if (place % 2 == 0) == near else -1)) % count
        pairs.append((work_of(gx, gy), work_of(*((other, gy) if dim == 0 else (gx, other)))))
    return pairs


def swapped(block, even, dim):
    first = lax.slice_in_dim(block, 0, 2, axis=dim + 1)
    last = lax.slice_in_dim(block, 4, 6, axis=dim + 1)
    far = lax.ppermute(jnp.where(even, first, last), ALL, partners(dim, False))
    near = lax.ppermute(jnp.where(even, last, first), ALL, partners(dim, True))
    low = jnp.where(even, far, near)
    high = jnp.where(even, near, far)
    return jnp.concatenate([low, block, high], axis=dim + 1)


def padded(block):
    odd_x = lax.axis_index("gx_0") + lax.axis_index("gx_1") + lax.axis_index("gy_0")
    odd_y = odd_x + lax.axis_index("gy_2")
    block = swapped(block, odd_x % 2 == 0, 0)
    return swapped(block, odd_y % 2 == 0, 1)


def local(position, velocity, other_accel, phase_ids, counts):
    slot_index = jnp.arange(128, dtype=jnp.int32)
    live = slot_index[None, None, :] < counts[:, :, None]
    code = jnp.where(live, phase_ids + 1, 0).astype(F32)
    masks = jnp.asarray(offset_masks(), BF16)
    rest = position - 0.5 + TIME_STEP * (velocity + TIME_STEP * other_accel)
    base = jnp.stack([jnp.where(live, rest[0], FAR), jnp.where(live, rest[1], 0.0)], axis=2)
    packed = to_work(jnp.concatenate([base, code[:, :, None, :]], axis=2))
    base = packed[:, :, :2]
    first = padded(packed[None])[0]
    near = first[:, :, :2]
    code8 = first[1:9, 1:9, 2]
    own8 = jnp.pad(packed[:, :, 2], ((1, 1), (1, 1), (0, 0)))
    pressure = jnp.zeros((8, 8, 128), F32)
    rows = []
    for iteration in range(ITERS):
        last = iteration == ITERS - 1
        bounds, sums, gain = call_kdf(near, jnp.zeros_like(base) if last else base, code8, own8, pressure, masks)
        seen = lax.all_to_all(bounds, ALL, 0, 0, tiled=True)
        if not last:
            wide = padded(sums)
            near, pressure, row = call_kc(seen, wide, code8, pressure, gain)
            rows.append(row)
    parts = jnp.stack([sums[0, :, :, 0], sums[0, :, :, 1], sums[1, :, :, 0], sums[1, :, :, 1], sums[2, :, :, 0], sums[2, :, :, 1],
                       pressure[1:7, 1:7], gain[1:7, 1:7]])
    parts = to_home(parts)
    return call_kz(seen, parts, position, velocity, other_accel, code, rows)


def solution(mesh):
    torus = Mesh(mesh.devices.reshape(4, 2, 2, 4, 2), ("gx_0", "gx_1", "gy_0", "gy_1", "gy_2"))
    in_specs = (
        P(None, GX, GY, None),
        P(None, GX, GY, None),
        P(None, GX, GY, None),
        P(GX, GY, None),
        P(GX, GY),
    )
    out_specs = (P(None, GX, GY, None), P(None, GX, GY, None), P(GX, GY, None), P())
    return jax.shard_map(local, mesh=torus, in_specs=in_specs, out_specs=out_specs, check_vma=False)
```

```python
import jax
import jax.numpy as jnp
import numpy as np
from jax import lax
from jax.experimental import pallas as pl
from jax.experimental.pallas import tpu as pltpu
from jax.sharding import Mesh
from jax.sharding import PartitionSpec as P

ITERS = 4
GX = ("gx_0", "gx_1")
GY = ("gy_0", "gy_1", "gy_2")
ALL = GX + GY

F32, BF16 = jnp.float32, jnp.bfloat16
OFFS = tuple((ox, oy) for ox in (-1, 0, 1) for oy in (-1, 0, 1))


def offset_masks():
    out = np.ones((9, 32, 128), np.float32)
    for k, (ox, oy) in enumerate(OFFS):
        for row in (6, 7, 12, 13, 14, 15, 18, 19, 20, 21, 22, 23):
            out[k, row] = (ox, oy)[row % 2]
        out[k, 31] = ox * ox + oy * oy
    return out


def rnd(v):
    return v.astype(BF16).astype(F32)


def row_iota():
    return lax.broadcasted_iota(jnp.int32, (8, 128), 0)


def cell_slabs(pos_ref, r, c, want_l=True, want_r=True):
    row = row_iota()
    x = jnp.broadcast_to(pos_ref[r, c, 0:1, :], (8, 128))
    y = jnp.broadcast_to(pos_ref[r, c, 1:2, :], (8, 128))
    v = jnp.where((row & 1) == 1, y, x)
    v1 = rnd(v)
    rest = v - v1
    v2 = rnd(rest)
    v3 = rest - v2
    n = x * x + y * y
    n1 = rnd(n)
    nrest = n - n1
    n2 = rnd(nrest)
    n3 = nrest - n2
    left = right = None
    if want_l:
        la = v1
        lb = jnp.where((row == 4) | (row == 5), 1.0, v2)
        lc = jnp.where((row >= 2) & (row <= 5), 1.0, v3)
        ld = jnp.where(row == 0, n1, jnp.where(row == 1, n2, jnp.where(row == 2, n3, 1.0)))
        left = jnp.concatenate([la, lb, lc, ld], axis=0)
    if want_r:
        t1, t2, t3 = 2.0 * v1, 2.0 * v2, 2.0 * v3
        ra = jnp.where(row < 2, t1, jnp.where(row < 4, t2, jnp.where(row < 6, t3, -2.0)))
        rb = ra
        rc = jnp.where(row < 4, t1, jnp.where(row < 6, t2, -2.0))
        rd = jnp.where(row < 3, -1.0, jnp.where(row == 3, -n1, jnp.where(row == 4, -n2, jnp.where(row == 5, -n3, jnp.where(row == 6, 1.0, -1.0)))))
        right = jnp.concatenate([ra, rb, rc, rd], axis=0)
    return left, right


def pair_rhs(r1, r2, mask):
    zero = jnp.zeros((32, 128), BF16)
    return jnp.concatenate(
        [jnp.concatenate([r1 * mask, zero], axis=1), jnp.concatenate([zero, r2 * mask], axis=1)], axis=0)


def pair_s(left_t, rhs):
    return jnp.dot(left_t, rhs, preferred_element_type=F32)


def fill_slabs(pos_ref, ls, rs, lo, hi, rlo, rhi):
    def body(r, carry):
        for c in range(lo, hi):
            left, right = cell_slabs(pos_ref, r, c, True, rlo <= c < rhi)
            ls[r, c] = left
            if rlo <= c < rhi:
                rs[r, c] = right.astype(BF16)
        return carry
    lax.fori_loop(lo, hi, body, 0)


def fill_pairs(ls, lt, start, rows, cols, dr, dc, rbase, cbase):
    for i in range(rows):
        for j in range(cols):
            both = jnp.concatenate([ls[rbase + i, cbase + j], ls[rbase + i + dr, cbase + j + dc]], axis=0)
            lt[start + i * cols + j] = both.T.astype(BF16)


def density_pair(rs, lt, masks_ref, i1, i2, first, stride, squares=None, at=0):
    r1, r2 = rs[i1[0], i1[1]], rs[i2[0], i2[1]]
    acc = jnp.zeros((8, 256), F32)
    for k, (ox, oy) in enumerate(OFFS):
        s = pair_s(lt[first + ox * stride + oy], pair_rhs(r1, r2, masks_ref[k]))
        w = jnp.maximum(s, 0.0)
        w2 = w * w
        if squares is not None:
            squares[at * 9 + k] = w2
        w3 = w2 * w
        acc = acc + w3.reshape(16, 8, 256).sum(axis=0)
    return acc.sum(axis=0, keepdims=True)


OWN, RING, FP = 9, 7, 6
TIME_STEP = 0.05
KERNEL_NORM = 4.0 / (3.141592653589793 * 64.0)
SENTINEL = 1.0e30


def bounds_of(dens, code, bnd_ref):
    ratio = dens * jnp.where(code == 2.0, KERNEL_NORM / 1.5, KERNEL_NORM / 1.2)
    picks = []
    for phase in (1.0, 2.0):
        picks.append(jnp.where(code == phase, ratio, -SENTINEL))
    for phase in (1.0, 2.0):
        picks.append(jnp.where(code == phase, -ratio, -SENTINEL))
    lane = lax.broadcasted_iota(jnp.int32, (1, 128), 1)
    out = jnp.zeros((1, 128), F32)
    for k, pick in enumerate(picks):
        top = pick.max(axis=0).max(axis=0, keepdims=True).max(axis=1, keepdims=True)
        out = jnp.where(lane == k, top, out)
    bnd_ref[...] = jnp.broadcast_to(out, (128, 128))


def term_rows(t_ref, r, c):
    row = row_iota() & 3
    a, b0, b1 = (jnp.broadcast_to(t_ref[k, r, pl.ds(c, 1), :], (8, 128)) for k in range(3))
    return jnp.where(row == 0, 1.0, jnp.where(row == 1, a, jnp.where(row == 2, b0, b1)))


def hi_lo(v):
    hi = rnd(v)
    return jnp.where(row_iota() < 4, hi, v - hi)


def cell_moments(pos_ref, t_ref, r, c):
    t = term_rows(t_ref, r, c)
    x = jnp.broadcast_to(pos_ref[r + 1, c + 1, 0:1, :], (8, 128))
    y = jnp.broadcast_to(pos_ref[r + 1, c + 1, 1:2, :], (8, 128))
    groups = [hi_lo(t)]
    for q in (x, y):
        for o in (-1.0, 0.0, 1.0):
            groups.append(hi_lo(t * (q + o)))
    return groups


def kdf_kernel(pos_ref, base_ref, code_ref, own_ref, p_ref, masks_ref, bnd_ref, s_ref, q_ref, ls, rs, lt, dn, tt, gt, squares):
    fill_slabs(pos_ref, ls, rs, 0, 10, 1, 9)
    fill_pairs(ls, lt, 0, 5, 8, 3, 0, 1, 1)
    fill_pairs(ls, lt, 40, 3, 10, 7, 0, 0, 0)
    fill_pairs(ls, lt, 70, 8, 3, 0, 7, 1, 0)
    def own(step, carry):
        for u in range(OWN):
            n = step * OWN + u
            a, b = (u % 3, step * (OWN // 3) + u // 3) if OWN % 3 == 0 else (n % 3, n // 3)
            row = density_pair(rs, lt, masks_ref, (a + 2, b + 2), (a + 5, b + 2), (a + 1) * 8 + b + 1, 8, squares, n)
            dn[a + 1, pl.ds(b + 1, 1), :] = row[:, :128]
            dn[a + 4, pl.ds(b + 1, 1), :] = row[:, 128:]
        return carry
    lax.fori_loop(0, 18 // OWN, own, 0)
    def ring(step, carry):
        for u in range(RING):
            n = step * RING + u
            flat = n < 8
            r1, r2, c1, c2 = (jnp.where(flat, p, q) for p, q in ((1, n - 6), (8, n - 6), (n + 1, 1), (n + 1, 8)))
            row = density_pair(rs, lt, masks_ref, (r1, c1), (r2, c2), jnp.where(flat, n + 51, 3 * n + 50), jnp.where(flat, 10, 3))
            dn[r1 - 1, pl.ds(c1 - 1, 1), :] = row[:, :128]
            dn[r2 - 1, pl.ds(c2 - 1, 1), :] = row[:, 128:]
        return carry
    lax.fori_loop(0, 14 // RING, ring, 0)
    bounds_of(dn[...], own_ref[...], bnd_ref)
    code = code_ref[...]
    live = code > 0.0
    heavy = code == 2.0
    density = KERNEL_NORM * dn[...]
    ratio = density * jnp.where(heavy, 1.0 / 1.5, 1.0 / 1.2)
    q = jnp.where(live, jnp.where(heavy, 200.0, 100.0) * (ratio - 1.0), 0.0)
    q_ref[...] = q
    safe = jnp.where(live, density, 1.0)
    inv = jnp.where(live, 1.0 / (safe * safe), 0.0)
    b = q * inv
    tt[0] = p_ref[...] * inv
    tt[1] = jnp.where(heavy, 0.0, b)
    tt[2] = jnp.where(heavy, b, 0.0)
    def moments(i, carry):
        for j in range(8):
            one = cell_moments(pos_ref, tt, i, j)
            two = cell_moments(pos_ref, tt, i + 3, j)
            tiles = [jnp.concatenate([g, h], axis=0) for g, h in zip(one, two)]
            gt[i * 8 + j] = jnp.concatenate(tiles, axis=0).astype(BF16)
        return carry
    lax.fori_loop(0, 5, moments, 0)
    row = row_iota()
    def forces(step, carry):
        accs = [jnp.zeros((48, 256), F32) for _ in range(FP)]
        work = [((FP * step + m) % 3, (FP * step + m) // 3) for m in range(FP)]
        for k, (ox, oy) in enumerate(OFFS):
            for m in range(FP):
                a, bcol = work[m]
                p = (a + 1 + ox) * 8 + bcol + 1 + oy
                w2 = squares[(FP * step + m) * 9 + k]
                hi = w2.astype(BF16)
                lo = (w2 - hi.astype(F32)).astype(BF16)
                g = jnp.concatenate([gt[p, 0:16], gt[p, 32 + 16 * ox:48 + 16 * ox], gt[p, 80 + 16 * oy:96 + 16 * oy]], axis=0)
                accs[m] = accs[m] + jnp.dot(jnp.concatenate([g, g], axis=1), jnp.concatenate([hi, lo], axis=0), preferred_element_type=F32)
        for m in range(FP):
            a, bcol = work[m]
            acc = accs[m]
            for h in range(2):
                aa = a + 3 * h
                lanes = slice(128 * h, 128 * h + 128)
                sums = []
                for t in range(3):
                    m = acc[16 * t + 8 * h:16 * t + 8 * h + 8, lanes]
                    sums.append(m + jnp.concatenate([m[4:8], m[0:4]], axis=0))
                x = jnp.broadcast_to(pos_ref[aa + 2, bcol + 2, 0:1, :], (8, 128))
                y = jnp.broadcast_to(pos_ref[aa + 2, bcol + 2, 1:2, :], (8, 128))
                ex = x * sums[0] - sums[1]
                ey = y * sums[0] - sums[2]
                e = jnp.where(row < 4, ex, ey)
                e0 = jnp.where(row < 4, jnp.broadcast_to(ex[0:1], (8, 128)), jnp.broadcast_to(ey[0:1], (8, 128)))
                code_row = jnp.broadcast_to(code_ref[aa + 1, pl.ds(bcol + 1, 1), :], (8, 128))
                scale = 6.0 * KERNEL_NORM * TIME_STEP * TIME_STEP
                coef = jnp.where(code_row == 2.0, scale / 1.5, jnp.where(code_row == 1.0, scale, 0.0))
                out = coef * (term_rows(tt, aa + 1, bcol + 1) * e0 + e)
                s_ref[0, aa, bcol, 0:1, :] = base_ref[aa, bcol, 0:1, :] + out[1:2]
                s_ref[0, aa, bcol, 1:2, :] = base_ref[aa, bcol, 1:2, :] + out[5:6]
                for t in (1, 2):
                    s_ref[t, aa, bcol, 0:1, :] = out[t + 1:t + 2]
                    s_ref[t, aa, bcol, 1:2, :] = out[t + 5:t + 6]
        return carry
    lax.fori_loop(0, 18 // FP, forces, 0)


def kc_kernel(seen_ref, s_ref, code_ref, p_ref, q_ref, pos_ref, pout_ref, row_ref):
    top = seen_ref[...].max(axis=0, keepdims=True)
    lane = lax.broadcasted_iota(jnp.int32, (1, 128), 1)
    top0, top1, neg0, neg1 = (jnp.sum(jnp.where(lane == k, top, 0.0), axis=1, keepdims=True) for k in range(4))
    r0 = 1.0 / (1.0 + top0 + neg0)
    r1 = 1.0 / (1.0 + top1 + neg1)
    row_ref[...] = jnp.where(lane < 2, top, jnp.where(lane < 4, -top, jnp.where(lane == 4, r0, r1)))
    for a in range(8):
        pout_ref[a] = p_ref[a] + jnp.where(code_ref[a] == 2.0, r1, r0) * q_ref[a]
    for a in range(10):
        pos_ref[a] = s_ref[0, a] + r0[None] * s_ref[1, a] + r1[None] * s_ref[2, a]


VM = pl.BlockSpec(memory_space=pltpu.VMEM)


def shaped(shape, dtype=F32):
    return jax.ShapeDtypeStruct(shape, dtype)


def call_kdf(pos, base, code8, own8, p8, masks):
    return pl.pallas_call(
        kdf_kernel,
        out_shape=(shaped((128, 128)), shaped((3, 6, 6, 2, 128)), shaped((8, 8, 128))),
        in_specs=[VM] * 6, out_specs=(VM,) * 3,
        scratch_shapes=[pltpu.VMEM((10, 10, 32, 128), F32), pltpu.VMEM((10, 10, 32, 128), BF16), pltpu.VMEM((94, 128, 64), BF16),
                        pltpu.VMEM((8, 8, 128), F32), pltpu.VMEM((3, 8, 8, 128), F32), pltpu.VMEM((40, 112, 128), BF16),
                        pltpu.VMEM((162, 128, 256), F32)],
        compiler_params=pltpu.CompilerParams(vmem_limit_bytes=40 * 1024 * 1024),
        cost_estimate=pl.CostEstimate(flops=40_000_000, bytes_accessed=400_000, transcendentals=0),
        name="sweep")(pos, base, code8, own8, p8, masks)


def call_kc(seen, sums, code8, p8, gain):
    return pl.pallas_call(
        kc_kernel,
        out_shape=(shaped((10, 10, 2, 128)), shaped((8, 8, 128)), shaped((1, 128))),
        in_specs=[VM] * 5, out_specs=(VM,) * 3,
        compiler_params=pltpu.CompilerParams(vmem_limit_bytes=8 * 1024 * 1024),
        cost_estimate=pl.CostEstimate(flops=1_000_000, bytes_accessed=400_000, transcendentals=0),
        name="combine")(seen.reshape(128, 128), sums, code8, p8, gain)


def kz_kernel(seen_ref, parts_ref, pos_ref, vel_ref, acc_ref, code_ref, a_ref, b_ref, c_ref, npos_ref, nvel_ref, press_ref, mon_ref):
    top = seen_ref[...].max(axis=0, keepdims=True)
    lane = lax.broadcasted_iota(jnp.int32, (1, 128), 1)
    top0, top1, neg0, neg1 = (jnp.sum(jnp.where(lane == k, top, 0.0), axis=1, keepdims=True) for k in range(4))
    r0 = (1.0 / (1.0 + top0 + neg0))[None]
    r1 = (1.0 / (1.0 + top1 + neg1))[None]
    row = jnp.where(lane < 2, top, -top)
    mon_ref[...] = jnp.concatenate([a_ref[...], b_ref[...], c_ref[...], row], axis=0)[:, :4]
    code = code_ref[...]
    live = code > 0.0
    for c in range(2):
        delta = parts_ref[c] + r0 * parts_ref[2 + c] + r1 * parts_ref[4 + c]
        speed = jnp.where(live, vel_ref[c] + TIME_STEP * acc_ref[c] + delta * (1.0 / TIME_STEP), 0.0)
        place = jnp.where(live, pos_ref[c] + TIME_STEP * speed, 0.0)
        for a in range(6):
            for b in range(6):
                nvel_ref[a, b, c:c + 1, :] = speed[a, b:b + 1]
                npos_ref[a, b, c:c + 1, :] = place[a, b:b + 1]
    press_ref[...] = parts_ref[6] + jnp.where(code == 2.0, r1, r0) * parts_ref[7]


def call_kz(seen, parts, position, velocity, other_accel, code, rows):
    return pl.pallas_call(
        kz_kernel,
        out_shape=(shaped((6, 6, 2, 128)), shaped((6, 6, 2, 128)), shaped((6, 6, 128)), shaped((4, 4))),
        in_specs=[VM] * 9, out_specs=(VM,) * 4,
        compiler_params=pltpu.CompilerParams(vmem_limit_bytes=8 * 1024 * 1024),
        cost_estimate=pl.CostEstimate(flops=1_000_000, bytes_accessed=400_000, transcendentals=0),
        name="finish")(seen.reshape(128, 128), parts, position, velocity, other_accel, code, *rows)


FAR = 2.0 ** 20
TILES = [(gx, gy) for gx in range(8) for gy in range(16)]


def home_of(gx, gy):
    return gx * 16 + gy


def work_of(gx, gy):
    x = gx >> 1
    flip = (gx ^ x) & 1
    chip = gy >> 1
    high = chip >> 2
    y = chip & 3 if high == 0 else 3 - (chip & 3)
    return ((x * 2 + (flip ^ high)) * 2 + high) * 8 + y * 2 + ((gx + gy) & 1)


def to_work(block):
    return lax.ppermute(block, ALL, [(home_of(gx, gy), work_of(gx, gy)) for gx, gy in TILES])


def to_home(block):
    return lax.ppermute(block, ALL, [(work_of(gx, gy), home_of(gx, gy)) for gx, gy in TILES])


def partners(dim, near):
    pairs = []
    for gx, gy in TILES:
        place, count = ((gx, 8), (gy, 16))[dim]
        other = (place + (1 if (place % 2 == 0) == near else -1)) % count
        pairs.append((work_of(gx, gy), work_of(*((other, gy) if dim == 0 else (gx, other)))))
    return pairs


def swapped(block, even, dim):
    first = lax.slice_in_dim(block, 0, 2, axis=dim + 1)
    last = lax.slice_in_dim(block, 4, 6, axis=dim + 1)
    far = lax.ppermute(jnp.where(even, first, last), ALL, partners(dim, False))
    near = lax.ppermute(jnp.where(even, last, first), ALL, partners(dim, True))
    low = jnp.where(even, far, near)
    high = jnp.where(even, near, far)
    return jnp.concatenate([low, block, high], axis=dim + 1)


def padded(block):
    odd_x = lax.axis_index("gx_0") + lax.axis_index("gx_1") + lax.axis_index("gy_0")
    odd_y = odd_x + lax.axis_index("gy_2")
    block = swapped(block, odd_x % 2 == 0, 0)
    return swapped(block, odd_y % 2 == 0, 1)


def local(position, velocity, other_accel, phase_ids, counts):
    slot_index = jnp.arange(128, dtype=jnp.int32)
    live = slot_index[None, None, :] < counts[:, :, None]
    code = jnp.where(live, phase_ids + 1, 0).astype(F32)
    masks = jnp.asarray(offset_masks(), BF16)
    rest = position - 0.5 + TIME_STEP * (velocity + TIME_STEP * other_accel)
    base = jnp.stack([jnp.where(live, rest[0], FAR), jnp.where(live, rest[1], 0.0)], axis=2)
    packed = to_work(jnp.concatenate([base, code[:, :, None, :]], axis=2))
    base = packed[:, :, :2]
    first = padded(packed[None])[0]
    near = first[:, :, :2]
    code8 = first[1:9, 1:9, 2]
    own8 = jnp.pad(packed[:, :, 2], ((1, 1), (1, 1), (0, 0)))
    pressure = jnp.zeros((8, 8, 128), F32)
    rows = []
    for iteration in range(ITERS):
        last = iteration == ITERS - 1
        bounds, sums, gain = call_kdf(near, jnp.zeros_like(base) if last else base, code8, own8, pressure, masks)
        seen = lax.all_to_all(bounds, ALL, 0, 0, tiled=True)
        if not last:
            wide = padded(sums)
            near, pressure, row = call_kc(seen, wide, code8, pressure, gain)
            rows.append(row)
    parts = jnp.stack([sums[0, :, :, 0], sums[0, :, :, 1], sums[1, :, :, 0], sums[1, :, :, 1], sums[2, :, :, 0], sums[2, :, :, 1],
                       pressure[1:7, 1:7], gain[1:7, 1:7]])
    parts = to_home(parts)
    new_position, new_velocity, new_pressure, monitor = call_kz(seen, parts, position, velocity, other_accel, code, rows)
    return new_position.transpose((2, 0, 1, 3)), new_velocity.transpose((2, 0, 1, 3)), new_pressure, monitor


def solution(mesh):
    torus = Mesh(mesh.devices.reshape(4, 2, 2, 4, 2), ("gx_0", "gx_1", "gy_0", "gy_1", "gy_2"))
    in_specs = (
        P(None, GX, GY, None),
        P(None, GX, GY, None),
        P(None, GX, GY, None),
        P(GX, GY, None),
        P(GX, GY),
    )
    out_specs = (P(None, GX, GY, None), P(None, GX, GY, None), P(GX, GY, None), P())
    return jax.shard_map(local, mesh=torus, in_specs=in_specs, out_specs=out_specs, check_vma=False)
```
